32 devices in a mesh: fsdp: 8 (over y, x, core), sp: 4 (over z).
Axes of the slice: x: 2, y: 2, z: 4, core: 2. Of those that a mesh axis runs over, the one named last changes fastest.
Arguments:
- hidden_in: bfloat16 [8192, 2048], P(('fsdp', 'sp')), may hold values from -6 to 6
- positions: int32 [8192], P(('fsdp', 'sp')), may hold values from 0 to 1023, as said below
- attn_gain: float32 [2048], replicated, may hold values from 0.5 to 1.5
- qkv_weight: bfloat16 [4096, 2048], P('fsdp'), may hold values from -0.125 to 0.125
- query_gain: float32 [128], replicated, may hold values from 0.5 to 1.5
- key_gain: float32 [128], replicated, may hold values from 0.5 to 1.5
- out_weight: bfloat16 [2048, 2048], P('fsdp'), may hold values from -0.75 to 0.75
- mlp_gain: float32 [2048], replicated, may hold values from 0.5 to 1.5
- gate_up_weight: bfloat16 [12288, 2048], P('fsdp'), may hold values from -0.125 to 0.125
- down_weight: bfloat16 [2048, 6144], P('fsdp'), may hold values from -0.078125 to 0.078125
- cotangent: bfloat16 [8192, 2048], P(('fsdp', 'sp')), may hold values from -6 to 6
Outputs:
- hidden_out: bfloat16 [8192, 2048], P(('fsdp', 'sp'))
- grad_input: float32 [8192, 2048], P(('fsdp', 'sp'))
- grad_attn_gain: float32 [2048], replicated
- grad_qkv: float32 [4096, 2048], P('fsdp')
- grad_query_gain: float32 [128], replicated
- grad_key_gain: float32 [128], replicated
- grad_out: float32 [2048, 2048], P('fsdp')
- grad_mlp_gain: float32 [2048], replicated
- grad_gate_up: float32 [12288, 2048], P('fsdp')
- grad_down: float32 [2048, 6144], P('fsdp')
The draws below stay inside these ranges and needn't reach their ends.
Inputs may be any that keep to these rules, and one draw needn't show every extreme that they name: Within each sequence of 1024 tokens the positions count up by one from 0 and restart at 0 at most once; the first sequence counts from 0 to 1023 without a restart.
All inputs are finite; a program needn't handle non-finite values.
Results may differ from the reference program's by a relative error of at most 0.02.
Values may be sent and summed in bfloat16 or wider, within the bound.
A program may use at most 576 MiB of HBM per device.

```python
import jax
import jax.numpy as jnp
from jax import lax

D = 2048
H = 16
KV = 8
HD = 128
FF = 6144
SEQ_LEN = 1024
TOKENS = 8192


def draw_positions(key, part):
    count = TOKENS // SEQ_LEN
    splits = jax.random.randint(jax.random.fold_in(key, 11), (count,), 1, SEQ_LEN)
    index = jnp.arange(count)
    splits = jnp.where(index == 0, SEQ_LEN, splits)
    within = jnp.arange(SEQ_LEN)
    restarted = jnp.where(within[None, :] >= splits[:, None], within[None, :] - splits[:, None], within[None, :])
    return restarted.reshape(TOKENS).astype(jnp.int32)


def strengthened(array, stream_key, source, target, blocks, factor):
    def block_of(axis_at):
        return (jnp.arange(array.shape[axis_at]) // (array.shape[axis_at] // blocks)).reshape((-1,) + (1,) * (array.ndim - 1 - axis_at))

    one_side = jax.random.permutation(stream_key, blocks)[block_of(target)]
    second = (block_of(target) + blocks // 2) % blocks
    return jnp.where((block_of(source) == one_side) | (block_of(source) == second), factor * array, array)


def level_of(rng, dims, cuts, smallest, high):
    level = 1.0
    for axis_at, blocks in cuts:
        steps = jax.random.uniform(jax.random.fold_in(jax.random.fold_in(rng, 6), axis_at), (blocks,), jnp.float32, smallest / len(cuts), high / len(cuts))
        level = level * jnp.repeat(jnp.exp(steps), dims[axis_at] // blocks).reshape((-1,) + (1,) * (len(dims) - 1 - axis_at))
    return level


def bell_draw(own_key, dims, spread, most, shards=(), kind=jnp.bfloat16):
    values = spread * jax.random.normal(own_key, dims, jnp.float32)
    if shards:
        values = values * level_of(own_key, dims, shards, -0.22, 0.18)
    return jnp.clip(values, -most, most).astype(kind)


def noise_with(own_key, dims, width, most, pieces, heavy, kind=jnp.bfloat16):
    drawn = width * jax.random.normal(own_key, dims, jnp.float32)
    if pieces:
        drawn = drawn * level_of(own_key, dims, pieces, -0.22, 0.18)
    return jnp.clip(strengthened(drawn, jax.random.fold_in(own_key, 3), *heavy), -most, most).astype(kind)


def setup_inputs(seed: int = 0) -> dict:
    streams_of = jax.random.split(jax.random.key(seed), 12)
    return {
        "hidden_in": bell_draw(streams_of[0], (TOKENS, D), 1.0, 6.0, ((0, 32),)),
        "positions": draw_positions(jax.random.fold_in(streams_of[11], 71), 0),
        "attn_gain": jnp.clip(1.0 + 0.1 * jax.random.normal(streams_of[2], (D,), jnp.float32), 0.5, 1.5),
        "qkv_weight": bell_draw(streams_of[3], ((H + 2 * KV) * HD, D), D ** -0.5, 0.125, ((0, 8),)),
        "query_gain": jnp.clip(1.0 + 0.1 * jax.random.normal(streams_of[4], (HD,), jnp.float32), 0.5, 1.5),
        "key_gain": jnp.clip(1.0 + 0.1 * jax.random.normal(streams_of[5], (HD,), jnp.float32), 0.5, 1.5),
        "out_weight": bell_draw(streams_of[6], (D, H * HD), (H * HD // 32) ** -0.5, 0.75, ((0, 8),)),
        "mlp_gain": jnp.clip(1.0 + 0.1 * jax.random.normal(streams_of[7], (D,), jnp.float32), 0.5, 1.5),
        "gate_up_weight": bell_draw(streams_of[8], (2 * FF, D), D ** -0.5, 0.125, ((0, 8),)),
        "down_weight": bell_draw(streams_of[9], (D, FF), FF ** -0.5, 0.078125, ((0, 8),)),
        "cotangent": noise_with(streams_of[10], (TOKENS, D), 1.0, 6.0, ((0, 32),), (0, 1, 32, 2.75)),
    }


EPS = 1e-06
THETA = 1000000.0
NEGATIVE = -1e+30

def rms_forward(values, gain):
    inverse = lax.rsqrt(lax.optimization_barrier(jnp.mean(values * values, axis=-1, keepdims=True)) + EPS)
    return (values * inverse * gain, inverse)

def rms_backward(values, inverse, gain, upstream):
    scaled = upstream * gain
    cubed = inverse * inverse * inverse
    gradient = inverse * scaled - values * cubed * lax.optimization_barrier(jnp.mean(scaled * values, axis=-1, keepdims=True))
    return (gradient, upstream * values * inverse)

def rotary_tables(positions):
    half = HD // 2
    frequency = THETA ** (-(jnp.arange(half, dtype=jnp.float32) * 2.0 / HD))
    angle = positions.astype(jnp.float32)[:, None] * frequency[None, :]
    cosine = jnp.cos(angle)
    sine = jnp.sin(angle)
    return (jnp.concatenate([cosine, cosine], -1)[:, None, :], jnp.concatenate([sine, sine], -1)[:, None, :])

def rotate(values, cosine, sine):
    half = HD // 2
    turned = jnp.concatenate([-values[..., half:], values[..., :half]], -1)
    return values * cosine + turned * sine

def rotate_back(gradient, cosine, sine):
    half = HD // 2
    scaled = gradient * sine
    return gradient * cosine + jnp.concatenate([scaled[..., half:], -scaled[..., :half]], -1)

def scores_block(query_block, keys, start, block):
    factor = HD ** (-0.5)
    scores = jnp.einsum('qhd,khd->hqk', query_block.astype(jnp.float32), keys.astype(jnp.float32)) * factor
    query_rows = start + jnp.arange(block).astype(jnp.int32)
    key_rows = jnp.arange(keys.shape[0]).astype(jnp.int32)
    allowed = key_rows[None, :] <= query_rows[:, None]
    return jnp.where(allowed[None], scores, NEGATIVE)

def attention_forward(query, keys, values):
    length = query.shape[0]
    block = min(512, length)

    def one_block(index):
        start = (index * block).astype(jnp.int32)
        query_block = lax.dynamic_slice_in_dim(query, start, block, 0)
        scores = scores_block(query_block, keys, start, block)
        top = lax.optimization_barrier(jnp.max(scores, axis=-1, keepdims=True))
        logsum = top + jnp.log(lax.optimization_barrier(jnp.sum(jnp.exp(scores - top), axis=-1, keepdims=True)))
        weights = jnp.exp(scores - logsum).astype(jnp.bfloat16)
        mixed = jnp.einsum('hqk,khd->qhd', weights.astype(jnp.float32), values.astype(jnp.float32))
        return (mixed.astype(jnp.bfloat16), logsum[..., 0])
    mixed_all, logsums = lax.map(one_block, jnp.arange(length // block).astype(jnp.int32))
    return (mixed_all.reshape(query.shape), logsums)

def attention_backward(query, keys, values, mixed_all, logsums, grad_mixed):
    length = query.shape[0]
    block = min(512, length)
    factor = HD ** (-0.5)

    def one_block(carry, inputs):
        index, logsum = inputs
        start = (index * block).astype(jnp.int32)
        query_block = lax.dynamic_slice_in_dim(query, start, block, 0)
        grad_block = lax.dynamic_slice_in_dim(grad_mixed, start, block, 0)
        mixed_block = lax.dynamic_slice_in_dim(mixed_all, start, block, 0)
        scores = scores_block(query_block, keys, start, block)
        chances = jnp.exp(scores - logsum[..., None])
        weights_low = chances.astype(jnp.bfloat16)
        delta = lax.optimization_barrier(jnp.sum(grad_block.astype(jnp.float32) * mixed_block.astype(jnp.float32), axis=-1))
        grad_weights = jnp.einsum('qhd,khd->hqk', grad_block.astype(jnp.float32), values.astype(jnp.float32))
        grad_scores = (chances * (grad_weights - delta.T[:, :, None])).astype(jnp.bfloat16)
        grad_query = jnp.einsum('hqk,khd->qhd', grad_scores.astype(jnp.float32), keys.astype(jnp.float32)) * factor
        key_total = carry[0] + jnp.einsum('hqk,qhd->khd', grad_scores.astype(jnp.float32), query_block.astype(jnp.float32)) * factor
        value_total = carry[1] + jnp.einsum('hqk,qhd->khd', weights_low.astype(jnp.float32), grad_block.astype(jnp.float32))
        return ((key_total, value_total), grad_query)
    zeros = jnp.zeros(keys.shape, jnp.float32)
    totals, grad_query = lax.scan(one_block, (zeros, zeros), (jnp.arange(length // block).astype(jnp.int32), logsums))
    return (grad_query.reshape(query.shape), totals[0], totals[1])

def reference(hidden_in, positions, attn_gain, qkv_weight, query_gain, key_gain, out_weight, mlp_gain, gate_up_weight, down_weight, cotangent):
    count = TOKENS // SEQ_LEN
    group = H // KV
    f32 = jnp.float32
    low = jnp.bfloat16

    def one_sequence(carry, inputs):
        hidden_seq, position_seq, cotangent_seq = inputs
        hidden = hidden_seq.astype(f32)
        normed1, inverse1 = rms_forward(hidden, attn_gain)
        normed1_low = normed1.astype(low)
        projected = jnp.dot(normed1_low, qkv_weight.T, preferred_element_type=f32)
        query = projected[:, :H * HD].reshape(SEQ_LEN, H, HD)
        key = projected[:, H * HD:(H + KV) * HD].reshape(SEQ_LEN, KV, HD)
        value_low = projected[:, (H + KV) * HD:].astype(low).reshape(SEQ_LEN, KV, HD)
        cosine, sine = rotary_tables(position_seq)
        query_normed, query_inverse = rms_forward(query, query_gain)
        key_normed, key_inverse = rms_forward(key, key_gain)
        query_low = rotate(query_normed, cosine, sine).astype(low)
        key_low = rotate(key_normed, cosine, sine).astype(low)
        keys_all = jnp.repeat(key_low, group, axis=1)
        values_all = jnp.repeat(value_low, group, axis=1)
        mixed_all, logsums = attention_forward(query_low, keys_all, values_all)
        attended = mixed_all.reshape(SEQ_LEN, H * HD)
        middle = hidden + jnp.dot(attended, out_weight.T, preferred_element_type=f32)
        normed2, inverse2 = rms_forward(middle, mlp_gain)
        normed2_low = normed2.astype(low)
        gate_up = jnp.dot(normed2_low, gate_up_weight.T, preferred_element_type=f32)
        gate = gate_up[:, :FF]
        upper = gate_up[:, FF:]
        sigmoid = jax.nn.sigmoid(gate)
        activation = (gate * sigmoid * upper).astype(low)
        hidden_out = (middle + jnp.dot(activation, down_weight.T, preferred_element_type=f32)).astype(low)
        upstream = cotangent_seq.astype(f32)
        grad_down = jnp.dot(cotangent_seq.T, activation, preferred_element_type=f32)
        grad_act = jnp.dot(cotangent_seq, down_weight, preferred_element_type=f32)
        grad_gate = grad_act * upper * sigmoid * (1.0 + gate * (1.0 - sigmoid))
        grad_upper = grad_act * gate * sigmoid
        grad_gate_up_low = jnp.concatenate([grad_gate, grad_upper], 1).astype(low)
        grad_gate_up = jnp.dot(grad_gate_up_low.T, normed2_low, preferred_element_type=f32)
        grad_normed2 = jnp.dot(grad_gate_up_low, gate_up_weight, preferred_element_type=f32)
        back_two, mlp_term = rms_backward(middle, inverse2, mlp_gain, grad_normed2)
        grad_middle = upstream + back_two
        grad_mixed_low = grad_middle.astype(low)
        grad_out = jnp.dot(grad_mixed_low.T, attended, preferred_element_type=f32)
        grad_attended = jnp.dot(grad_mixed_low, out_weight, preferred_element_type=f32).astype(low).reshape(SEQ_LEN, H, HD)
        grad_query_rot, grad_keys, grad_values = attention_backward(query_low, keys_all, values_all, mixed_all, logsums, grad_attended)
        grad_key_rot = grad_keys.reshape(SEQ_LEN, KV, group, HD).sum(2).astype(low)
        grad_value_low = grad_values.reshape(SEQ_LEN, KV, group, HD).sum(2).astype(low)
        grad_query_low = grad_query_rot.astype(low)
        grad_query, query_term = rms_backward(query, query_inverse, query_gain, rotate_back(grad_query_low.astype(f32), cosine, sine))
        grad_key, key_term = rms_backward(key, key_inverse, key_gain, rotate_back(grad_key_rot.astype(f32), cosine, sine))
        grad_projected = jnp.concatenate([grad_query.reshape(SEQ_LEN, H * HD), grad_key.reshape(SEQ_LEN, KV * HD), grad_value_low.reshape(SEQ_LEN, KV * HD).astype(f32)], 1).astype(low)
        grad_qkv = jnp.dot(grad_projected.T, normed1_low, preferred_element_type=f32)
        grad_normed1 = jnp.dot(grad_projected, qkv_weight, preferred_element_type=f32)
        back_one, attn_term = rms_backward(hidden, inverse1, attn_gain, grad_normed1)
        grad_input = grad_middle + back_one
        terms = (lax.optimization_barrier(jnp.sum(attn_term, axis=0)), grad_qkv, lax.optimization_barrier(jnp.sum(query_term, axis=(0, 1))), lax.optimization_barrier(jnp.sum(key_term, axis=(0, 1))), grad_out, lax.optimization_barrier(jnp.sum(mlp_term, axis=0)), grad_gate_up, grad_down)
        updated = tuple((before + extra for before, extra in zip(carry, terms)))
        return (updated, (hidden_out, grad_input))
    start = (jnp.zeros((D,), f32), jnp.zeros(qkv_weight.shape, f32), jnp.zeros((HD,), f32), jnp.zeros((HD,), f32), jnp.zeros(out_weight.shape, f32), jnp.zeros((D,), f32), jnp.zeros(gate_up_weight.shape, f32), jnp.zeros(down_weight.shape, f32))
    inputs = (hidden_in.reshape(count, SEQ_LEN, D), positions.reshape(count, SEQ_LEN), cotangent.reshape(count, SEQ_LEN, D))
    totals, results = lax.scan(one_sequence, start, inputs)
    hidden_out = results[0].reshape(TOKENS, D)
    grad_input = results[1].reshape(TOKENS, D)
    return (hidden_out, grad_input, totals[0], totals[1], totals[2], totals[3], totals[4], totals[5], totals[6], totals[7])
```

```python
import functools

import jax
import jax.numpy as jnp
from jax import lax
from jax.sharding import PartitionSpec as P


H = 16
KV = 8
HD = 128
FF = 6144


EPS = 1e-06
THETA = 1000000.0
NEGATIVE = -1e30


def rms_forward(values, gain):
    inverse = lax.rsqrt(jnp.mean(values * values, axis=-1, keepdims=True) + EPS)
    return (values * inverse * gain, inverse)


def rms_backward(values, inverse, gain, upstream):
    scaled = upstream * gain
    cubed = inverse * inverse * inverse
    gradient = inverse * scaled - values * cubed * jnp.mean(scaled * values, axis=-1, keepdims=True)
    return (gradient, upstream * values * inverse)


def rotary_tables(positions):
    half = HD // 2
    frequency = THETA ** (-(jnp.arange(half, dtype=jnp.float32) * 2.0 / HD))
    angle = positions.astype(jnp.float32)[:, None] * frequency[None, :]
    cosine = jnp.cos(angle)
    sine = jnp.sin(angle)
    return (
        jnp.concatenate([cosine, cosine], -1)[:, None, :],
        jnp.concatenate([sine, sine], -1)[:, None, :],
    )


def rotate(values, cosine, sine):
    half = HD // 2
    turned = jnp.concatenate([-values[..., half:], values[..., :half]], -1)
    return values * cosine + turned * sine


def rotate_back(gradient, cosine, sine):
    half = HD // 2
    scaled = gradient * sine
    return gradient * cosine + jnp.concatenate([scaled[..., half:], -scaled[..., :half]], -1)


def scores_block(query_block, keys, start):
    scores = jnp.einsum("qhd,khd->hqk", query_block, keys, preferred_element_type=jnp.float32)
    query_rows = start + jnp.arange(query_block.shape[0])
    key_rows = jnp.arange(keys.shape[0])
    allowed = key_rows[None, :] <= query_rows[:, None]
    return jnp.where(allowed[None], scores * HD ** (-0.5), NEGATIVE)


def blocks_of(length):
    block = min(512, length)
    return [(start, start + block) for start in range(0, length, block)]


def attention_forward(query, keys, values):
    mixed_all, logsums = [], []
    for start, stop in blocks_of(query.shape[0]):
        scores = scores_block(query[start:stop], keys[:stop], start)
        top = jnp.max(scores, axis=-1, keepdims=True)
        logsum = top + jnp.log(jnp.sum(jnp.exp(scores - top), axis=-1, keepdims=True))
        weights = jnp.exp(scores - logsum).astype(jnp.bfloat16)
        mixed = jnp.einsum(
            "hqk,khd->qhd", weights, values[:stop], preferred_element_type=jnp.float32
        )
        mixed_all.append(mixed.astype(jnp.bfloat16))
        logsums.append(logsum)
    return (jnp.concatenate(mixed_all, 0), logsums)


def attention_backward(query, keys, values, mixed_all, logsums, grad_mixed, between):
    length = query.shape[0]
    factor = HD ** (-0.5)
    grad_query, key_total, value_total = [], None, None
    for (start, stop), logsum in reversed(list(zip(blocks_of(length), logsums))):
        query_block = query[start:stop]
        grad_block = grad_mixed[start:stop]
        mixed_block = mixed_all[start:stop]
        scores = scores_block(query_block, keys[:stop], start)
        chances = jnp.exp(scores - logsum)
        weights_low = chances.astype(jnp.bfloat16)
        delta = jnp.sum(grad_block.astype(jnp.float32) * mixed_block.astype(jnp.float32), axis=-1)
        grad_weights = jnp.einsum(
            "qhd,khd->hqk", grad_block, values[:stop], preferred_element_type=jnp.float32
        )
        grad_scores = (chances * (grad_weights - delta.T[:, :, None])).astype(jnp.bfloat16)
        grad_query.append(
            jnp.einsum(
                "hqk,khd->qhd", grad_scores, keys[:stop], preferred_element_type=jnp.float32
            )
            * factor
        )
        key_part = (
            jnp.einsum(
                "hqk,qhd->khd", grad_scores, query_block, preferred_element_type=jnp.float32
            )
            * factor
        )
        value_part = jnp.einsum(
            "hqk,qhd->khd", weights_low, grad_block, preferred_element_type=jnp.float32
        )
        if key_total is None:
            key_total, value_total = key_part, value_part
            between(grad_query[0])
        else:
            key_total = key_total.at[:stop].add(key_part)
            value_total = value_total.at[:stop].add(value_part)
    return (jnp.concatenate(grad_query[::-1], 0), key_total, value_total)


def gather_rows(array):
    return lax.all_gather(array, "fsdp", axis=0, tiled=True)


def product_nt(inputs, weight):
    return lax.dot_general(
        inputs, weight, (((1,), (1,)), ((), ())), preferred_element_type=jnp.float32
    )


def product_tn(left, right):
    return lax.dot_general(
        left, right, (((0,), (0,)), ((), ())), preferred_element_type=jnp.float32
    )


def scatter_sum(partial):
    return lax.psum_scatter(
        partial.astype(jnp.bfloat16), "fsdp", scatter_dimension=0, tiled=True
    ).astype(jnp.float32)


class Chain:
    def __init__(self, partial, count):
        half = count // 2
        self.count = count
        self.value = partial.astype(jnp.bfloat16)
        self.hops = []
        if count % 2 == 0:
            for s in range(half - 1):
                self.hops.append(([(s, s + 1), (count - 1 - s, count - 2 - s)], None))
            self.hops.append(([(half - 1, half), (half, half - 1)], None))
            for s in reversed(range(half - 1)):
                self.hops.append(([(s + 1, s), (count - 2 - s, count - 1 - s)], s))
        elif count > 1:
            self.value = lax.psum(self.value, "sp")
        self.at = 0
        self.send()

    def send(self):
        if self.at < len(self.hops):
            self.flying = lax.ppermute(self.value, "sp", self.hops[self.at][0])

    def advance(self):
        if self.at >= len(self.hops):
            return
        arrived = self.flying
        depth = self.hops[self.at][1]
        if depth is None:
            total = self.value.astype(jnp.float32) + arrived.astype(jnp.float32)
            self.value = total.astype(jnp.bfloat16)
        else:
            place = lax.axis_index("sp")
            mine = jnp.minimum(place, self.count - 1 - place) == depth
            self.value = jnp.where(mine, arrived, self.value)
        self.at += 1
        self.send()

    def finish(self):
        while self.at < len(self.hops):
            self.advance()
        return self.value


def halves(array):
    middle = array.shape[0] // 2
    return (array[:middle], array[middle:])


def layer(
    ways,
    line,
    hidden_in,
    positions,
    attn_gain,
    qkv_weight,
    query_gain,
    key_gain,
    out_weight,
    mlp_gain,
    gate_up_weight,
    down_weight,
    cotangent,
):
    f32 = jnp.float32
    low = jnp.bfloat16
    rows, width = hidden_in.shape
    group = H // KV
    units = FF // ways
    pairs_of = ways // 2
    side = lax.axis_index("fsdp") // pairs_of
    swap = [(f, (f + pairs_of) % ways) for f in range(ways)]

    qkv_full = gather_rows(qkv_weight)
    qkv_full, gate_up_late, down_late, out_late, cotangent_late = lax.optimization_barrier(
        (qkv_full, gate_up_weight, down_weight, out_weight, cotangent)
    )
    out_full = gather_rows(out_late)
    cotangent_all = gather_rows(cotangent_late)
    kept = lax.dynamic_slice_in_dim(gate_up_late, side * units, units, 0)
    sent = lax.dynamic_slice_in_dim(gate_up_late, (1 - side) * units, units, 0)
    swapped = lax.ppermute(sent, "fsdp", swap)
    gate_up_own = jnp.concatenate([kept, swapped], 0)
    down_split = down_late.reshape(-1, pairs_of, 2, units).transpose(2, 1, 0, 3)
    down_turned = lax.all_to_all(
        down_split.reshape(ways, -1, units), "fsdp", split_axis=0, concat_axis=0, tiled=True
    )
    hidden = hidden_in.astype(f32)
    normed1, inverse1 = rms_forward(hidden, attn_gain)
    normed1_low = normed1.astype(low)
    projected = product_nt(normed1_low, qkv_full)
    query = projected[:, : H * HD].reshape(rows, H, HD)
    key = projected[:, H * HD : (H + KV) * HD].reshape(rows, KV, HD)
    value_low = projected[:, (H + KV) * HD :].astype(low)
    cosine, sine = rotary_tables(positions)
    query_normed, query_inverse = rms_forward(query, query_gain)
    key_normed, key_inverse = rms_forward(key, key_gain)
    query_low = rotate(query_normed, cosine, sine).astype(low).reshape(rows, H * HD)
    key_low = rotate(key_normed, cosine, sine).astype(low).reshape(rows, KV * HD)
    query_low, key_low, value_low, down_turned = lax.optimization_barrier(
        (query_low, key_low, value_low, down_turned)
    )
    down_own = down_turned.reshape(width, units)
    query_heads, key_heads, value_heads = (
        lax.all_to_all(query_low, "sp", split_axis=1, concat_axis=0, tiled=True),
        lax.all_to_all(key_low, "sp", split_axis=1, concat_axis=0, tiled=True),
        lax.all_to_all(value_low, "sp", split_axis=1, concat_axis=0, tiled=True),
    )
    length = query_heads.shape[0]
    local_kv = key_heads.shape[1] // HD
    query_local = query_heads.reshape(length, -1, HD)
    keys_local = jnp.repeat(key_heads.reshape(length, local_kv, HD), group, axis=1)
    values_local = jnp.repeat(value_heads.reshape(length, local_kv, HD), group, axis=1)
    mixed_heads, logsums = attention_forward(query_local, keys_local, values_local)
    attended = lax.all_to_all(
        mixed_heads.reshape(length, -1), "sp", split_axis=0, concat_axis=1, tiled=True
    )
    middle = hidden + product_nt(attended, out_full)
    normed2, inverse2 = rms_forward(middle, mlp_gain)
    normed2_all = gather_rows(normed2.astype(low))
    normed1_late, middle = lax.optimization_barrier((normed1_low, middle))
    normed1_all = gather_rows(normed1_late)

    grad_act = jnp.dot(cotangent_all, down_own, preferred_element_type=f32)
    both = product_nt(normed2_all, gate_up_own)
    first, second = both[:, :units], both[:, units:]
    gate = jnp.where(side == 0, first, second)
    upper = jnp.where(side == 0, second, first)
    sigmoid = jax.nn.sigmoid(gate)
    activation = (gate * sigmoid * upper).astype(low)
    grad_gate = grad_act * upper * sigmoid * (1.0 + gate * (1.0 - sigmoid))
    grad_upper = grad_act * gate * sigmoid
    grad_first = jnp.where(side == 0, grad_gate, grad_upper).astype(low)
    grad_second = jnp.where(side == 0, grad_upper, grad_gate).astype(low)
    grad_both = jnp.concatenate([grad_first, grad_second], 1)
    grad_normed2 = scatter_sum(jnp.dot(grad_both, gate_up_own, preferred_element_type=f32))
    grad_kept = product_tn(grad_first, normed2_all).astype(low)
    grad_sent = product_tn(grad_second, normed2_all).astype(low)
    grad_down_own = product_tn(cotangent_all, activation).astype(low)
    kept_chains = [Chain(part, line) for part in halves(grad_kept)]
    grad_down_sum = lax.psum(grad_down_own, "sp")

    back_two, mlp_term = rms_backward(middle, inverse2, mlp_gain, grad_normed2)
    grad_middle = cotangent.astype(f32) + back_two
    grad_mixed_low = grad_middle.astype(low)
    grad_attended = jnp.dot(grad_mixed_low, out_full, preferred_element_type=f32).astype(low)
    grad_heads = lax.all_to_all(grad_attended, "sp", split_axis=1, concat_axis=0, tiled=True)
    grad_sent, grad_mixed_low = lax.optimization_barrier((grad_sent, grad_mixed_low))
    grad_out = scatter_sum(product_tn(grad_mixed_low, attended))
    sent_chains = [Chain(part, line) for part in halves(grad_sent)]
    for chain in kept_chains:
        chain.advance()

    def between(value):
        for chain in kept_chains:
            chain.advance()

    activation_late, grad_heads = lax.optimization_barrier((activation, grad_heads))
    hidden_out = (middle + scatter_sum(product_nt(activation_late, down_own))).astype(low)

    grad_query_local, grad_keys, grad_values = attention_backward(
        query_local,
        keys_local,
        values_local,
        mixed_heads,
        logsums,
        grad_heads.reshape(length, -1, HD),
        between,
    )
    grad_query_send = grad_query_local.astype(low).reshape(length, -1)
    grad_key_send = (
        grad_keys.reshape(length, local_kv, group, HD).sum(2).astype(low).reshape(length, -1)
    )
    grad_value_send = (
        grad_values.reshape(length, local_kv, group, HD).sum(2).astype(low).reshape(length, -1)
    )
    for chain in sent_chains:
        chain.advance()
    grad_query_low, grad_key_low, grad_value_low = (
        lax.all_to_all(grad_query_send, "sp", split_axis=0, concat_axis=1, tiled=True),
        lax.all_to_all(grad_key_send, "sp", split_axis=0, concat_axis=1, tiled=True),
        lax.all_to_all(grad_value_send, "sp", split_axis=0, concat_axis=1, tiled=True),
    )
    grad_query, query_term = rms_backward(
        query,
        query_inverse,
        query_gain,
        rotate_back(grad_query_low.astype(f32).reshape(rows, H, HD), cosine, sine),
    )
    grad_key, key_term = rms_backward(
        key,
        key_inverse,
        key_gain,
        rotate_back(grad_key_low.astype(f32).reshape(rows, KV, HD), cosine, sine),
    )
    grad_projected = jnp.concatenate(
        [
            grad_query.reshape(rows, H * HD).astype(low),
            grad_key.reshape(rows, KV * HD).astype(low),
            grad_value_low,
        ],
        1,
    )
    grad_columns = lax.all_to_all(grad_projected, "fsdp", split_axis=1, concat_axis=0, tiled=True)
    for chain in sent_chains:
        chain.advance()
    grad_qkv_own = product_tn(grad_columns, normed1_all)
    qkv_chains = [Chain(part, line) for part in halves(grad_qkv_own)]
    out_chain = Chain(grad_out, line)
    grad_normed1 = jnp.dot(grad_projected, qkv_full, preferred_element_type=f32)
    back_one, attn_term = rms_backward(hidden, inverse1, attn_gain, grad_normed1)
    grad_input = grad_middle + back_one
    grad_kept = jnp.concatenate([chain.finish() for chain in kept_chains], 0)
    grad_sent = jnp.concatenate([chain.finish() for chain in sent_chains], 0)
    grad_swapped = lax.ppermute(grad_sent, "fsdp", swap)
    grad_gate_up = jnp.concatenate(
        [
            jnp.where(side == 0, grad_kept, grad_swapped),
            jnp.where(side == 0, grad_swapped, grad_kept),
        ],
        0,
    ).astype(f32)
    grad_down_sum, grad_projected = lax.optimization_barrier((grad_down_sum, grad_projected))
    down_back = lax.all_to_all(
        grad_down_sum.reshape(ways, -1, units),
        "fsdp",
        split_axis=0,
        concat_axis=0,
        tiled=True,
    )
    grad_down = (
        down_back.reshape(2, pairs_of, -1, units)
        .transpose(2, 1, 0, 3)
        .reshape(down_weight.shape)
        .astype(f32)
    )
    grad_out = out_chain.finish().astype(f32)
    grad_qkv = jnp.concatenate([chain.finish() for chain in qkv_chains], 0).astype(f32)
    terms = jnp.concatenate(
        [
            jnp.sum(attn_term, axis=0),
            jnp.sum(mlp_term, axis=0),
            jnp.sum(query_term, axis=(0, 1)),
            jnp.sum(key_term, axis=(0, 1)),
        ]
    )
    all_terms = lax.all_gather(terms.reshape(1, -1), ("fsdp", "sp"), axis=0, tiled=True)
    sums = jnp.sum(all_terms, axis=0)
    gains = (
        sums[:width],
        sums[2 * width : 2 * width + HD],
        sums[2 * width + HD :],
        sums[width : 2 * width],
    )
    return (
        hidden_out,
        grad_input,
        gains[0],
        grad_qkv,
        gains[1],
        gains[2],
        grad_out,
        gains[3],
        grad_gate_up,
        grad_down,
    )


def solution(mesh):
    return jax.shard_map(
        functools.partial(layer, mesh.shape["fsdp"], mesh.shape["sp"]),
        mesh=mesh,
        in_specs=(
            P(("fsdp", "sp"), None),
            P(("fsdp", "sp")),
            P(),
            P("fsdp", None),
            P(),
            P(),
            P("fsdp", None),
            P(),
            P("fsdp", None),
            P("fsdp", None),
            P(("fsdp", "sp"), None),
        ),
        out_specs=(
            P(("fsdp", "sp"), None),
            P(("fsdp", "sp"), None),
            P(),
            P("fsdp", None),
            P(),
            P(),
            P("fsdp", None),
            P(),
            P("fsdp", None),
            P("fsdp", None),
        ),
        check_vma=False,
    )
```

```python
import functools

import jax
import jax.numpy as jnp
from jax import lax
from jax.sharding import PartitionSpec as P


H = 16
KV = 8
HD = 128
FF = 6144


EPS = 1e-06
THETA = 1000000.0
NEGATIVE = -1e30


def rms_forward(values, gain):
    inverse = lax.rsqrt(jnp.mean(values * values, axis=-1, keepdims=True) + EPS)
    return (values * inverse * gain, inverse)


def rms_backward(values, inverse, gain, upstream):
    scaled = upstream * gain
    cubed = inverse * inverse * inverse
    gradient = inverse * scaled - values * cubed * jnp.mean(scaled * values, axis=-1, keepdims=True)
    return (gradient, upstream * values * inverse)


def rotary_tables(positions):
    half = HD // 2
    frequency = THETA ** (-(jnp.arange(half, dtype=jnp.float32) * 2.0 / HD))
    angle = positions.astype(jnp.float32)[:, None] * frequency[None, :]
    cosine = jnp.cos(angle)
    sine = jnp.sin(angle)
    return (
        jnp.concatenate([cosine, cosine], -1)[:, None, :],
        jnp.concatenate([sine, sine], -1)[:, None, :],
    )


def rotate(values, cosine, sine):
    half = HD // 2
    turned = jnp.concatenate([-values[..., half:], values[..., :half]], -1)
    return values * cosine + turned * sine


def rotate_back(gradient, cosine, sine):
    half = HD // 2
    scaled = gradient * sine
    return gradient * cosine + jnp.concatenate([scaled[..., half:], -scaled[..., :half]], -1)


def scores_block(query_block, keys, start):
    scores = jnp.einsum("qhd,khd->hqk", query_block, keys, preferred_element_type=jnp.float32)
    query_rows = start + jnp.arange(query_block.shape[0])
    key_rows = jnp.arange(keys.shape[0])
    allowed = key_rows[None, :] <= query_rows[:, None]
    return jnp.where(allowed[None], scores * HD ** (-0.5), NEGATIVE)


def blocks_of(length):
    block = min(512, length)
    return [(start, start + block) for start in range(0, length, block)]


def attention_forward(query, keys, values):
    mixed_all, logsums = [], []
    for start, stop in blocks_of(query.shape[0]):
        scores = scores_block(query[start:stop], keys[:stop], start)
        top = jnp.max(scores, axis=-1, keepdims=True)
        logsum = top + jnp.log(jnp.sum(jnp.exp(scores - top), axis=-1, keepdims=True))
        weights = jnp.exp(scores - logsum).astype(jnp.bfloat16)
        mixed = jnp.einsum(
            "hqk,khd->qhd", weights, values[:stop], preferred_element_type=jnp.float32
        )
        mixed_all.append(mixed.astype(jnp.bfloat16))
        logsums.append(logsum)
    return (jnp.concatenate(mixed_all, 0), logsums)


def attention_backward(query, keys, values, mixed_all, logsums, grad_mixed, between):
    length = query.shape[0]
    factor = HD ** (-0.5)
    grad_query, key_total, value_total = [], None, None
    for (start, stop), logsum in reversed(list(zip(blocks_of(length), logsums))):
        query_block = query[start:stop]
        grad_block = grad_mixed[start:stop]
        mixed_block = mixed_all[start:stop]
        scores = scores_block(query_block, keys[:stop], start)
        chances = jnp.exp(scores - logsum)
        weights_low = chances.astype(jnp.bfloat16)
        delta = jnp.sum(grad_block.astype(jnp.float32) * mixed_block.astype(jnp.float32), axis=-1)
        grad_weights = jnp.einsum(
            "qhd,khd->hqk", grad_block, values[:stop], preferred_element_type=jnp.float32
        )
        grad_scores = (chances * (grad_weights - delta.T[:, :, None])).astype(jnp.bfloat16)
        grad_query.append(
            jnp.einsum(
                "hqk,khd->qhd", grad_scores, keys[:stop], preferred_element_type=jnp.float32
            )
            * factor
        )
        key_part = (
            jnp.einsum(
                "hqk,qhd->khd", grad_scores, query_block, preferred_element_type=jnp.float32
            )
            * factor
        )
        value_part = jnp.einsum(
            "hqk,qhd->khd", weights_low, grad_block, preferred_element_type=jnp.float32
        )
        if key_total is None:
            key_total, value_total = key_part, value_part
            grad_mixed, key_total = between((grad_mixed, key_total))
        else:
            key_total = key_total.at[:stop].add(key_part)
            value_total = value_total.at[:stop].add(value_part)
    return (jnp.concatenate(grad_query[::-1], 0), key_total, value_total)


def gather_rows(array):
    return lax.all_gather(array, "fsdp", axis=0, tiled=True)


def product_nt(inputs, weight):
    return lax.dot_general(
        inputs, weight, (((1,), (1,)), ((), ())), preferred_element_type=jnp.float32
    )


def product_tn(left, right):
    return lax.dot_general(
        left, right, (((0,), (0,)), ((), ())), preferred_element_type=jnp.float32
    )


def scatter_sum(partial):
    return lax.psum_scatter(
        partial.astype(jnp.bfloat16), "fsdp", scatter_dimension=0, tiled=True
    ).astype(jnp.float32)


class Chain:
    def __init__(self, partial, count):
        half = count // 2
        self.count = count
        self.value = partial.astype(jnp.bfloat16)
        self.flying = None
        self.hops = []
        if count % 2 == 0:
            for s in range(half - 1):
                self.hops.append(([(s, s + 1), (count - 1 - s, count - 2 - s)], None))
            self.hops.append(([(half - 1, half), (half, half - 1)], None))
            for s in reversed(range(half - 1)):
                self.hops.append(([(s + 1, s), (count - 2 - s, count - 1 - s)], s))
        elif count > 1:
            self.value = lax.psum(self.value, "sp")
        self.at = 0

    def send(self):
        if self.at < len(self.hops):
            self.flying = lax.ppermute(self.value, "sp", self.hops[self.at][0])

    def take(self):
        depth = self.hops[self.at][1]
        if depth is None:
            total = self.value.astype(jnp.float32) + self.flying.astype(jnp.float32)
            self.value = total.astype(jnp.bfloat16)
        else:
            place = lax.axis_index("sp")
            mine = jnp.minimum(place, self.count - 1 - place) == depth
            self.value = jnp.where(mine, self.flying, self.value)
        self.at += 1
        self.flying = None

    def finish(self):
        while self.at < len(self.hops):
            if self.flying is None:
                self.send()
            self.take()
        return self.value


def meet(values, moving, starting=()):
    moving = [c for c in moving if c.flying is not None]
    tied = lax.optimization_barrier(
        (values, [c.flying for c in moving], [c.value for c in starting])
    )
    for chain, arrived in zip(moving, tied[1]):
        chain.flying = arrived
        chain.take()
        chain.send()
    for chain, value in zip(starting, tied[2]):
        chain.value = value
        chain.send()
    return tied[0]


def turn(blocks, ways):
    me = lax.axis_index("fsdp")
    result = lax.dynamic_update_slice_in_dim(
        jnp.zeros_like(blocks), lax.dynamic_slice_in_dim(blocks, me, 1, 0), me, 0
    )
    for shift in range(1, ways):
        block = lax.dynamic_slice_in_dim(blocks, (me + shift) % ways, 1, 0)
        pairs = [(f, (f + shift) % ways) for f in range(ways)]
        arrived = lax.ppermute(block, "fsdp", pairs)
        result = lax.dynamic_update_slice_in_dim(result, arrived, (me - shift) % ways, 0)
    return result


def sum_all(values, sizes):
    for axis, size in sizes:
        if size & (size - 1):
            values = lax.psum(values, axis)
            continue
        step = 1
        while step < size:
            values = values + lax.ppermute(values, axis, [(d, d ^ step) for d in range(size)])
            step *= 2
    return values


def halves(array):
    middle = array.shape[0] // 2
    return (array[:middle], array[middle:])


def layer(
    ways,
    line,
    hidden_in,
    positions,
    attn_gain,
    qkv_weight,
    query_gain,
    key_gain,
    out_weight,
    mlp_gain,
    gate_up_weight,
    down_weight,
    cotangent,
):
    f32 = jnp.float32
    low = jnp.bfloat16
    rows, width = hidden_in.shape
    group = H // KV
    units = FF // ways
    pairs_of = ways // 2
    side = lax.axis_index("fsdp") // pairs_of
    swap = [(f, (f + pairs_of) % ways) for f in range(ways)]

    qkv_full = gather_rows(qkv_weight)
    qkv_full, gate_up_late, down_late, out_late, cotangent_late = lax.optimization_barrier(
        (qkv_full, gate_up_weight, down_weight, out_weight, cotangent)
    )
    out_full = gather_rows(out_late)
    cotangent_all = gather_rows(cotangent_late)
    kept = lax.dynamic_slice_in_dim(gate_up_late, side * units, units, 0)
    sent = lax.dynamic_slice_in_dim(gate_up_late, (1 - side) * units, units, 0)
    swapped = lax.ppermute(sent, "fsdp", swap)
    gate_up_own = jnp.concatenate([kept, swapped], 0)
    down_split = down_late.reshape(-1, pairs_of, 2, units).transpose(2, 1, 0, 3)
    down_own = turn(down_split.reshape(ways, -1, units), ways).reshape(width, units)
    hidden = hidden_in.astype(f32)
    normed1, inverse1 = rms_forward(hidden, attn_gain)
    normed1_low = normed1.astype(low)
    projected = product_nt(normed1_low, qkv_full)
    query = projected[:, : H * HD].reshape(rows, H, HD)
    key = projected[:, H * HD : (H + KV) * HD].reshape(rows, KV, HD)
    value_low = projected[:, (H + KV) * HD :].astype(low)
    cosine, sine = rotary_tables(positions)
    query_normed, query_inverse = rms_forward(query, query_gain)
    key_normed, key_inverse = rms_forward(key, key_gain)
    query_low = rotate(query_normed, cosine, sine).astype(low).reshape(rows, H * HD)
    key_low = rotate(key_normed, cosine, sine).astype(low).reshape(rows, KV * HD)
    query_heads, key_heads, value_heads = (
        lax.all_to_all(query_low, "sp", split_axis=1, concat_axis=0, tiled=True),
        lax.all_to_all(key_low, "sp", split_axis=1, concat_axis=0, tiled=True),
        lax.all_to_all(value_low, "sp", split_axis=1, concat_axis=0, tiled=True),
    )
    length = query_heads.shape[0]
    local_kv = key_heads.shape[1] // HD
    query_local = query_heads.reshape(length, -1, HD)
    keys_local = jnp.repeat(key_heads.reshape(length, local_kv, HD), group, axis=1)
    values_local = jnp.repeat(value_heads.reshape(length, local_kv, HD), group, axis=1)
    mixed_heads, logsums = attention_forward(query_local, keys_local, values_local)
    attended = lax.all_to_all(
        mixed_heads.reshape(length, -1), "sp", split_axis=0, concat_axis=1, tiled=True
    )
    middle = hidden + product_nt(attended, out_full)
    normed2, inverse2 = rms_forward(middle, mlp_gain)
    normed2_all = gather_rows(normed2.astype(low))
    normed1_late, middle = lax.optimization_barrier((normed1_low, middle))
    normed1_all = gather_rows(normed1_late)

    grad_act = jnp.dot(cotangent_all, down_own, preferred_element_type=f32)
    both = product_nt(normed2_all, gate_up_own)
    first, second = both[:, :units], both[:, units:]
    gate = jnp.where(side == 0, first, second)
    upper = jnp.where(side == 0, second, first)
    sigmoid = jax.nn.sigmoid(gate)
    activation = (gate * sigmoid * upper).astype(low)
    grad_gate = grad_act * upper * sigmoid * (1.0 + gate * (1.0 - sigmoid))
    grad_upper = grad_act * gate * sigmoid
    grad_first = jnp.where(side == 0, grad_gate, grad_upper).astype(low)
    grad_second = jnp.where(side == 0, grad_upper, grad_gate).astype(low)
    grad_both = jnp.concatenate([grad_first, grad_second], 1)
    grad_normed2 = scatter_sum(jnp.dot(grad_both, gate_up_own, preferred_element_type=f32))
    grad_sent = product_tn(grad_second, normed2_all).astype(low)
    s0, s1 = (Chain(part, line) for part in halves(grad_sent))
    s0.send()
    s1.send()
    grad_down_own = product_tn(cotangent_all, activation).astype(low)
    grad_kept = product_tn(grad_first, normed2_all).astype(low)
    grad_kept, grad_down_own = meet((grad_kept, grad_down_own), [s0])
    d0, d1 = (Chain(part, line) for part in halves(grad_down_own))
    k0, k1 = (Chain(part, line) for part in halves(grad_kept))

    back_two, mlp_term = rms_backward(middle, inverse2, mlp_gain, grad_normed2)
    grad_middle = cotangent.astype(f32) + back_two
    grad_mixed_low = grad_middle.astype(low)
    grad_attended = jnp.dot(grad_mixed_low, out_full, preferred_element_type=f32).astype(low)
    grad_heads = lax.all_to_all(grad_attended, "sp", split_axis=1, concat_axis=0, tiled=True)
    grad_mixed_low = meet(grad_mixed_low, [s1], [d0])
    grad_out = scatter_sum(product_tn(grad_mixed_low, attended))
    grad_query_local, grad_keys, grad_values = attention_backward(
        query_local,
        keys_local,
        values_local,
        mixed_heads,
        logsums,
        grad_heads.reshape(length, -1, HD),
        lambda values: meet(values, [s0], [d1]),
    )
    grad_query_send = grad_query_local.astype(low).reshape(length, -1)
    grad_key_send = (
        grad_keys.reshape(length, local_kv, group, HD).sum(2).astype(low).reshape(length, -1)
    )
    grad_value_send = (
        grad_values.reshape(length, local_kv, group, HD).sum(2).astype(low).reshape(length, -1)
    )
    grads_send = jnp.concatenate([grad_query_send, grad_key_send, grad_value_send], 1)
    grads_send, activation = meet((grads_send, activation), [s1, d0], [k0])
    grads_low = lax.all_to_all(grads_send, "sp", split_axis=0, concat_axis=1, tiled=True)
    hidden_out = (middle + scatter_sum(product_nt(activation, down_own))).astype(low)
    grads_low = meet(grads_low, [s0, d1], [k1])
    grads_low = grads_low.reshape(rows, line, -1)
    cuts = (grad_query_send.shape[1], grad_query_send.shape[1] + grad_key_send.shape[1])
    grad_query_low = grads_low[:, :, : cuts[0]]
    grad_key_low = grads_low[:, :, cuts[0] : cuts[1]]
    grad_value_low = grads_low[:, :, cuts[1] :].reshape(rows, KV * HD)
    grad_query, query_term = rms_backward(
        query,
        query_inverse,
        query_gain,
        rotate_back(grad_query_low.astype(f32).reshape(rows, H, HD), cosine, sine),
    )
    grad_key, key_term = rms_backward(
        key,
        key_inverse,
        key_gain,
        rotate_back(grad_key_low.astype(f32).reshape(rows, KV, HD), cosine, sine),
    )
    grad_projected = jnp.concatenate(
        [
            grad_query.reshape(rows, H * HD).astype(low),
            grad_key.reshape(rows, KV * HD).astype(low),
            grad_value_low,
        ],
        1,
    )
    grad_columns = lax.all_to_all(grad_projected, "fsdp", split_axis=1, concat_axis=0, tiled=True)
    out_chain = Chain(grad_out, line)
    grad_columns = meet(grad_columns, [d0, k0, s1], [out_chain])
    grad_normed1 = jnp.dot(grad_projected, qkv_full, preferred_element_type=f32)
    grad_qkv_own = product_tn(grad_columns, normed1_all).astype(low)
    back_one, attn_term = rms_backward(hidden, inverse1, attn_gain, grad_normed1)
    grad_input = grad_middle + back_one
    terms = jnp.concatenate(
        [
            jnp.sum(attn_term, axis=0),
            jnp.sum(mlp_term, axis=0),
            jnp.sum(query_term, axis=(0, 1)),
            jnp.sum(key_term, axis=(0, 1)),
        ]
    )
    grad_qkv_own, terms = meet((grad_qkv_own, terms), [d1, k1])
    q0, q1 = (Chain(part, line) for part in halves(grad_qkv_own))
    q0.send()
    q1.send()
    sums = sum_all(terms, (("fsdp", ways), ("sp", line)))
    grad_swapped = []
    for chain in (s0, s1):
        grad_swapped.append(lax.ppermute(chain.finish(), "fsdp", swap))
    grad_swapped = jnp.concatenate(grad_swapped, 0)
    grad_down_sum = jnp.concatenate([d0.finish(), d1.finish()], 0)
    down_back = lax.all_to_all(
        grad_down_sum.reshape(ways, -1, units),
        "fsdp",
        split_axis=0,
        concat_axis=0,
        tiled=True,
    )
    grad_down = (
        down_back.reshape(2, pairs_of, -1, units)
        .transpose(2, 1, 0, 3)
        .reshape(down_weight.shape)
        .astype(f32)
    )
    grad_kept = jnp.concatenate([k0.finish(), k1.finish()], 0)
    grad_gate_up = jnp.concatenate(
        [
            jnp.where(side == 0, grad_kept, grad_swapped),
            jnp.where(side == 0, grad_swapped, grad_kept),
        ],
        0,
    ).astype(f32)
    grad_out = out_chain.finish().astype(f32)
    grad_qkv = jnp.concatenate([q0.finish(), q1.finish()], 0).astype(f32)
    gains = (
        sums[:width],
        sums[2 * width : 2 * width + HD],
        sums[2 * width + HD :],
        sums[width : 2 * width],
    )
    return (
        hidden_out,
        grad_input,
        gains[0],
        grad_qkv,
        gains[1],
        gains[2],
        grad_out,
        gains[3],
        grad_gate_up,
        grad_down,
    )


def solution(mesh):
    return jax.shard_map(
        functools.partial(layer, mesh.shape["fsdp"], mesh.shape["sp"]),
        mesh=mesh,
        in_specs=(
            P(("fsdp", "sp"), None),
            P(("fsdp", "sp")),
            P(),
            P("fsdp", None),
            P(),
            P(),
            P("fsdp", None),
            P(),
            P("fsdp", None),
            P("fsdp", None),
            P(("fsdp", "sp"), None),
        ),
        out_specs=(
            P(("fsdp", "sp"), None),
            P(("fsdp", "sp"), None),
            P(),
            P("fsdp", None),
            P(),
            P(),
            P("fsdp", None),
            P(),
            P("fsdp", None),
            P("fsdp", None),
        ),
        check_vma=False,
    )
```

```python
import functools

import jax
import jax.numpy as jnp
from jax import lax
from jax.sharding import PartitionSpec as P


H = 16
KV = 8
HD = 128
FF = 6144


EPS = 1e-06
THETA = 1000000.0
NEGATIVE = -1e30


def rms_forward(values, gain):
    inverse = lax.rsqrt(jnp.mean(values * values, axis=-1, keepdims=True) + EPS)
    return (values * inverse * gain, inverse)


def rms_backward(values, inverse, gain, upstream):
    scaled = upstream * gain
    cubed = inverse * inverse * inverse
    gradient = inverse * scaled - values * cubed * jnp.mean(scaled * values, axis=-1, keepdims=True)
    return (gradient, upstream * values * inverse)


def rotary_tables(positions):
    half = HD // 2
    frequency = THETA ** (-(jnp.arange(half, dtype=jnp.float32) * 2.0 / HD))
    angle = positions.astype(jnp.float32)[:, None] * frequency[None, :]
    cosine = jnp.cos(angle)
    sine = jnp.sin(angle)
    return (
        jnp.concatenate([cosine, cosine], -1)[:, None, :],
        jnp.concatenate([sine, sine], -1)[:, None, :],
    )


def rotate(values, cosine, sine):
    half = HD // 2
    turned = jnp.concatenate([-values[..., half:], values[..., :half]], -1)
    return values * cosine + turned * sine


def rotate_back(gradient, cosine, sine):
    half = HD // 2
    scaled = gradient * sine
    return gradient * cosine + jnp.concatenate([scaled[..., half:], -scaled[..., :half]], -1)


def scores_block(query_block, keys, start):
    scores = jnp.einsum("qhd,khd->hqk", query_block, keys, preferred_element_type=jnp.float32)
    query_rows = start + jnp.arange(query_block.shape[0])
    key_rows = jnp.arange(keys.shape[0])
    allowed = key_rows[None, :] <= query_rows[:, None]
    return jnp.where(allowed[None], scores * HD ** (-0.5), NEGATIVE)


def blocks_of(length):
    block = min(512, length)
    return [(start, start + block) for start in range(0, length, block)]


def attention_forward(query, keys, values):
    mixed_all, logsums = [], []
    for start, stop in blocks_of(query.shape[0]):
        scores = scores_block(query[start:stop], keys[:stop], start)
        top = jnp.max(scores, axis=-1, keepdims=True)
        logsum = top + jnp.log(jnp.sum(jnp.exp(scores - top), axis=-1, keepdims=True))
        weights = jnp.exp(scores - logsum).astype(jnp.bfloat16)
        mixed = jnp.einsum(
            "hqk,khd->qhd", weights, values[:stop], preferred_element_type=jnp.float32
        )
        mixed_all.append(mixed.astype(jnp.bfloat16))
        logsums.append(logsum)
    return (jnp.concatenate(mixed_all, 0), logsums)


def attention_backward(query, keys, values, mixed_all, logsums, grad_mixed, between):
    length = query.shape[0]
    factor = HD ** (-0.5)
    grad_query, key_total, value_total = [], None, None
    for (start, stop), logsum in reversed(list(zip(blocks_of(length), logsums))):
        query_block = query[start:stop]
        grad_block = grad_mixed[start:stop]
        mixed_block = mixed_all[start:stop]
        scores = scores_block(query_block, keys[:stop], start)
        chances = jnp.exp(scores - logsum)
        weights_low = chances.astype(jnp.bfloat16)
        delta = jnp.sum(grad_block.astype(jnp.float32) * mixed_block.astype(jnp.float32), axis=-1)
        grad_weights = jnp.einsum(
            "qhd,khd->hqk", grad_block, values[:stop], preferred_element_type=jnp.float32
        )
        grad_scores = (chances * (grad_weights - delta.T[:, :, None])).astype(jnp.bfloat16)
        grad_query.append(
            jnp.einsum(
                "hqk,khd->qhd", grad_scores, keys[:stop], preferred_element_type=jnp.float32
            )
            * factor
        )
        key_part = (
            jnp.einsum("hqk,qhd->khd", grad_scores, query_block, preferred_element_type=jnp.float32)
            * factor
        )
        value_part = jnp.einsum(
            "hqk,qhd->khd", weights_low, grad_block, preferred_element_type=jnp.float32
        )
        if key_total is None:
            key_total, value_total = key_part, value_part
            grad_mixed, key_total = between((grad_mixed, key_total))
        else:
            key_total = key_total.at[:stop].add(key_part)
            value_total = value_total.at[:stop].add(value_part)
    return (jnp.concatenate(grad_query[::-1], 0), key_total, value_total)


def gather_rows(array):
    return lax.all_gather(array, "fsdp", axis=0, tiled=True)


def product_nt(inputs, weight):
    return lax.dot_general(
        inputs, weight, (((1,), (1,)), ((), ())), preferred_element_type=jnp.float32
    )


def product_tn(left, right):
    return lax.dot_general(
        left, right, (((0,), (0,)), ((), ())), preferred_element_type=jnp.float32
    )


def scatter_sum(partial):
    return lax.psum_scatter(
        partial.astype(jnp.bfloat16), "fsdp", scatter_dimension=0, tiled=True
    ).astype(jnp.float32)


class Chain:
    def __init__(self, partial, count):
        half = count // 2
        self.count = count
        self.value = partial.astype(jnp.bfloat16)
        self.flying = None
        self.hops = []
        if count % 2 == 0:
            for s in range(half - 1):
                self.hops.append(([(s, s + 1), (count - 1 - s, count - 2 - s)], None))
            self.hops.append(([(half - 1, half), (half, half - 1)], None))
            for s in reversed(range(half - 1)):
                self.hops.append(([(s + 1, s), (count - 2 - s, count - 1 - s)], s))
        elif count > 1:
            self.value = lax.psum(self.value, "sp")
        self.at = 0

    def send(self):
        if self.at < len(self.hops):
            self.flying = lax.ppermute(self.value, "sp", self.hops[self.at][0])

    def take(self):
        depth = self.hops[self.at][1]
        if depth is None:
            total = self.value.astype(jnp.float32) + self.flying.astype(jnp.float32)
            self.value = total.astype(jnp.bfloat16)
        else:
            place = lax.axis_index("sp")
            mine = jnp.minimum(place, self.count - 1 - place) == depth
            self.value = jnp.where(mine, self.flying, self.value)
        self.at += 1
        self.flying = None

    def finish(self):
        while self.at < len(self.hops):
            if self.flying is None:
                self.send()
            self.take()
        return self.value


def meet(values, moving, starting=()):
    moving = [c for c in moving if c.flying is not None]
    tied = lax.optimization_barrier(
        (values, [c.flying for c in moving], [c.value for c in starting])
    )
    for chain, arrived in zip(moving, tied[1]):
        chain.flying = arrived
        chain.take()
        chain.send()
    for chain, value in zip(starting, tied[2]):
        chain.value = value
        chain.send()
    return tied[0]


def turn(blocks, ways):
    me = lax.axis_index("fsdp")
    result = lax.dynamic_update_slice_in_dim(
        jnp.zeros_like(blocks), lax.dynamic_slice_in_dim(blocks, me, 1, 0), me, 0
    )
    for shift in range(1, ways):
        block = lax.dynamic_slice_in_dim(blocks, (me + shift) % ways, 1, 0)
        pairs = [(f, (f + shift) % ways) for f in range(ways)]
        arrived = lax.ppermute(block, "fsdp", pairs)
        result = lax.dynamic_update_slice_in_dim(result, arrived, (me - shift) % ways, 0)
    return result


def sum_all(values, sizes):
    for axis, size in sizes:
        if size & (size - 1):
            values = lax.psum(values, axis)
            continue
        step = 1
        while step < size:
            values = values + lax.ppermute(values, axis, [(d, d ^ step) for d in range(size)])
            step *= 2
    return values


def halves(array):
    middle = array.shape[0] // 2
    return (array[:middle], array[middle:])


def layer(
    ways,
    line,
    hidden_in,
    positions,
    attn_gain,
    qkv_weight,
    query_gain,
    key_gain,
    out_weight,
    mlp_gain,
    gate_up_weight,
    down_weight,
    cotangent,
):
    f32 = jnp.float32
    low = jnp.bfloat16
    rows, width = hidden_in.shape
    group = H // KV
    units = FF // ways
    pairs_of = ways // 2
    side = lax.axis_index("fsdp") // pairs_of
    swap = [(f, (f + pairs_of) % ways) for f in range(ways)]

    qkv_full = gather_rows(qkv_weight)
    qkv_full, gate_up_late, down_late, out_late, cotangent_late = lax.optimization_barrier(
        (qkv_full, gate_up_weight, down_weight, out_weight, cotangent)
    )
    out_full = gather_rows(out_late)
    cotangent_all = gather_rows(cotangent_late)
    kept = lax.dynamic_slice_in_dim(gate_up_late, side * units, units, 0)
    sent = lax.dynamic_slice_in_dim(gate_up_late, (1 - side) * units, units, 0)
    swapped = lax.ppermute(sent, "fsdp", swap)
    gate_up_own = jnp.concatenate([kept, swapped], 0)
    down_split = down_late.reshape(-1, pairs_of, 2, units).transpose(2, 1, 0, 3)
    down_own = turn(down_split.reshape(ways, -1, units), ways).reshape(width, units)
    hidden = hidden_in.astype(f32)
    normed1, inverse1 = rms_forward(hidden, attn_gain)
    normed1_low = normed1.astype(low)
    projected = product_nt(normed1_low, qkv_full)
    query = projected[:, : H * HD].reshape(rows, H, HD)
    key = projected[:, H * HD : (H + KV) * HD].reshape(rows, KV, HD)
    value_low = projected[:, (H + KV) * HD :].astype(low)
    cosine, sine = rotary_tables(positions)
    query_normed, query_inverse = rms_forward(query, query_gain)
    key_normed, key_inverse = rms_forward(key, key_gain)
    query_low = rotate(query_normed, cosine, sine).astype(low).reshape(rows, H * HD)
    key_low = rotate(key_normed, cosine, sine).astype(low).reshape(rows, KV * HD)
    query_heads, key_heads, value_heads = (
        lax.all_to_all(query_low, "sp", split_axis=1, concat_axis=0, tiled=True),
        lax.all_to_all(key_low, "sp", split_axis=1, concat_axis=0, tiled=True),
        lax.all_to_all(value_low, "sp", split_axis=1, concat_axis=0, tiled=True),
    )
    length = query_heads.shape[0]
    local_kv = key_heads.shape[1] // HD
    query_local = query_heads.reshape(length, -1, HD)
    keys_local = jnp.repeat(key_heads.reshape(length, local_kv, HD), group, axis=1)
    values_local = jnp.repeat(value_heads.reshape(length, local_kv, HD), group, axis=1)
    mixed_heads, logsums = attention_forward(query_local, keys_local, values_local)
    attended = lax.all_to_all(
        mixed_heads.reshape(length, -1), "sp", split_axis=0, concat_axis=1, tiled=True
    )
    middle = hidden + product_nt(attended, out_full)
    normed2, inverse2 = rms_forward(middle, mlp_gain)
    normed2_all = gather_rows(normed2.astype(low))
    normed1_late, middle = lax.optimization_barrier((normed1_low, middle))
    normed1_all = gather_rows(normed1_late)

    grad_act = jnp.dot(cotangent_all, down_own, preferred_element_type=f32)
    both = product_nt(normed2_all, gate_up_own)
    first, second = both[:, :units], both[:, units:]
    gate = jnp.where(side == 0, first, second)
    upper = jnp.where(side == 0, second, first)
    sigmoid = jax.nn.sigmoid(gate)
    activation = (gate * sigmoid * upper).astype(low)
    grad_gate = grad_act * upper * sigmoid * (1.0 + gate * (1.0 - sigmoid))
    grad_upper = grad_act * gate * sigmoid
    grad_first = jnp.where(side == 0, grad_gate, grad_upper).astype(low)
    grad_second = jnp.where(side == 0, grad_upper, grad_gate).astype(low)
    grad_both = jnp.concatenate([grad_first, grad_second], 1)
    grad_normed2 = scatter_sum(jnp.dot(grad_both, gate_up_own, preferred_element_type=f32))
    grad_sent = product_tn(grad_second, normed2_all).astype(low)
    s0, s1 = (Chain(part, line) for part in halves(grad_sent))
    s0.send()
    s1.send()
    grad_down_own = product_tn(cotangent_all, activation).astype(low)
    grad_kept = product_tn(grad_first, normed2_all).astype(low)
    grad_kept, grad_down_own = meet((grad_kept, grad_down_own), [s0])
    d0, d1 = (Chain(part, line) for part in halves(grad_down_own))
    k0, k1 = (Chain(part, line) for part in halves(grad_kept))

    back_two, mlp_term = rms_backward(middle, inverse2, mlp_gain, grad_normed2)
    grad_middle = cotangent.astype(f32) + back_two
    grad_mixed_low = grad_middle.astype(low)
    grad_attended = jnp.dot(grad_mixed_low, out_full, preferred_element_type=f32).astype(low)
    grad_heads = lax.all_to_all(grad_attended, "sp", split_axis=1, concat_axis=0, tiled=True)
    grad_mixed_low = meet(grad_mixed_low, [s1], [d0, d1])
    grad_out = scatter_sum(product_tn(grad_mixed_low, attended))
    grad_query_local, grad_keys, grad_values = attention_backward(
        query_local,
        keys_local,
        values_local,
        mixed_heads,
        logsums,
        grad_heads.reshape(length, -1, HD),
        lambda values: meet(values, [s0]),
    )
    grad_query_send = grad_query_local.astype(low).reshape(length, -1)
    grad_key_send = (
        grad_keys.reshape(length, local_kv, group, HD).sum(2).astype(low).reshape(length, -1)
    )
    grad_value_send = (
        grad_values.reshape(length, local_kv, group, HD).sum(2).astype(low).reshape(length, -1)
    )
    grads_send = jnp.concatenate([grad_query_send, grad_key_send, grad_value_send], 1)
    grads_send, activation = meet((grads_send, activation), [s1, d0])
    grads_low = lax.all_to_all(grads_send, "sp", split_axis=0, concat_axis=1, tiled=True)
    hidden_out = (middle + scatter_sum(product_nt(activation, down_own))).astype(low)
    grads_low = meet(grads_low, [d1], [k0, k1])
    grads_low = grads_low.reshape(rows, line, -1)
    cuts = (grad_query_send.shape[1], grad_query_send.shape[1] + grad_key_send.shape[1])
    grad_query_low = grads_low[:, :, : cuts[0]]
    grad_key_low = grads_low[:, :, cuts[0] : cuts[1]]
    grad_value_low = grads_low[:, :, cuts[1] :].reshape(rows, KV * HD)
    grad_query, query_term = rms_backward(
        query,
        query_inverse,
        query_gain,
        rotate_back(grad_query_low.astype(f32).reshape(rows, H, HD), cosine, sine),
    )
    grad_query, query_term = meet((grad_query, query_term), [d0, k0])
    grad_key, key_term = rms_backward(
        key,
        key_inverse,
        key_gain,
        rotate_back(grad_key_low.astype(f32).reshape(rows, KV, HD), cosine, sine),
    )
    grad_projected = jnp.concatenate(
        [
            grad_query.reshape(rows, H * HD).astype(low),
            grad_key.reshape(rows, KV * HD).astype(low),
            grad_value_low,
        ],
        1,
    )
    grad_columns = lax.all_to_all(grad_projected, "fsdp", split_axis=1, concat_axis=0, tiled=True)
    out_chain = Chain(grad_out, line)
    grad_columns = meet(grad_columns, [d1, k1], [out_chain])
    grad_normed1 = jnp.dot(grad_projected, qkv_full, preferred_element_type=f32)
    grad_qkv_own = product_tn(grad_columns, normed1_all).astype(low)
    back_one, attn_term = rms_backward(hidden, inverse1, attn_gain, grad_normed1)
    grad_input = grad_middle + back_one
    terms = jnp.concatenate(
        [
            jnp.sum(attn_term, axis=0),
            jnp.sum(mlp_term, axis=0),
            jnp.sum(query_term, axis=(0, 1)),
            jnp.sum(key_term, axis=(0, 1)),
        ]
    )
    grad_qkv_own, terms = meet((grad_qkv_own, terms), [k0])
    q0, q1 = (Chain(part, line) for part in halves(grad_qkv_own))
    q0.send()
    q1.send()
    sums = sum_all(terms, (("fsdp", ways), ("sp", line)))
    grad_swapped = []
    for chain in (s0, s1):
        grad_swapped.append(lax.ppermute(chain.finish(), "fsdp", swap))
    grad_swapped = jnp.concatenate(grad_swapped, 0)
    grad_down_sum = jnp.concatenate([d0.finish(), d1.finish()], 0)
    down_back = lax.all_to_all(
        grad_down_sum.reshape(ways, -1, units),
        "fsdp",
        split_axis=0,
        concat_axis=0,
        tiled=True,
    )
    grad_down = (
        down_back.reshape(2, pairs_of, -1, units)
        .transpose(2, 1, 0, 3)
        .reshape(down_weight.shape)
        .astype(f32)
    )
    grad_kept = jnp.concatenate([k0.finish(), k1.finish()], 0)
    grad_gate_up = jnp.concatenate(
        [
            jnp.where(side == 0, grad_kept, grad_swapped),
            jnp.where(side == 0, grad_swapped, grad_kept),
        ],
        0,
    ).astype(f32)
    grad_out = out_chain.finish().astype(f32)
    grad_qkv = jnp.concatenate([q0.finish(), q1.finish()], 0).astype(f32)
    gains = (
        sums[:width],
        sums[2 * width : 2 * width + HD],
        sums[2 * width + HD :],
        sums[width : 2 * width],
    )
    return (
        hidden_out,
        grad_input,
        gains[0],
        grad_qkv,
        gains[1],
        gains[2],
        grad_out,
        gains[3],
        grad_gate_up,
        grad_down,
    )


def solution(mesh):
    return jax.shard_map(
        functools.partial(layer, mesh.shape["fsdp"], mesh.shape["sp"]),
        mesh=mesh,
        in_specs=(
            P(("fsdp", "sp"), None),
            P(("fsdp", "sp")),
            P(),
            P("fsdp", None),
            P(),
            P(),
            P("fsdp", None),
            P(),
            P("fsdp", None),
            P("fsdp", None),
            P(("fsdp", "sp"), None),
        ),
        out_specs=(
            P(("fsdp", "sp"), None),
            P(("fsdp", "sp"), None),
            P(),
            P("fsdp", None),
            P(),
            P(),
            P("fsdp", None),
            P(),
            P("fsdp", None),
            P("fsdp", None),
        ),
        check_vma=False,
    )
```

```python
import functools

import jax
import jax.numpy as jnp
from jax import lax
from jax.sharding import PartitionSpec as P


H = 16
KV = 8
HD = 128
FF = 6144


EPS = 1e-06
THETA = 1000000.0
NEGATIVE = -1e30


def rms_forward(values, gain):
    inverse = lax.rsqrt(jnp.mean(values * values, axis=-1, keepdims=True) + EPS)
    return (values * inverse * gain, inverse)


def rms_backward(values, inverse, gain, upstream):
    scaled = upstream * gain
    cubed = inverse * inverse * inverse
    gradient = inverse * scaled - values * cubed * jnp.mean(scaled * values, axis=-1, keepdims=True)
    return (gradient, upstream * values * inverse)


def rotary_tables(positions):
    half = HD // 2
    frequency = THETA ** (-(jnp.arange(half, dtype=jnp.float32) * 2.0 / HD))
    angle = positions.astype(jnp.float32)[:, None] * frequency[None, :]
    cosine = jnp.cos(angle)
    sine = jnp.sin(angle)
    return (
        jnp.concatenate([cosine, cosine], -1)[:, None, :],
        jnp.concatenate([sine, sine], -1)[:, None, :],
    )


def rotate(values, cosine, sine):
    half = HD // 2
    turned = jnp.concatenate([-values[..., half:], values[..., :half]], -1)
    return values * cosine + turned * sine


def rotate_back(gradient, cosine, sine):
    half = HD // 2
    scaled = gradient * sine
    return gradient * cosine + jnp.concatenate([scaled[..., half:], -scaled[..., :half]], -1)


def scores_block(query_block, keys, start):
    scores = jnp.einsum("qhd,khd->hqk", query_block, keys, preferred_element_type=jnp.float32)
    query_rows = start + jnp.arange(query_block.shape[0])
    key_rows = jnp.arange(keys.shape[0])
    allowed = key_rows[None, :] <= query_rows[:, None]
    return jnp.where(allowed[None], scores * HD ** (-0.5), NEGATIVE)


def blocks_of(length):
    block = min(512, length)
    return [(start, start + block) for start in range(0, length, block)]


def attention_forward(query, keys, values):
    mixed_all, logsums = [], []
    for start, stop in blocks_of(query.shape[0]):
        scores = scores_block(query[start:stop], keys[:stop], start)
        top = jnp.max(scores, axis=-1, keepdims=True)
        logsum = top + jnp.log(jnp.sum(jnp.exp(scores - top), axis=-1, keepdims=True))
        weights = jnp.exp(scores - logsum).astype(jnp.bfloat16)
        mixed = jnp.einsum(
            "hqk,khd->qhd", weights, values[:stop], preferred_element_type=jnp.float32
        )
        mixed_all.append(mixed.astype(jnp.bfloat16))
        logsums.append(logsum)
    return (jnp.concatenate(mixed_all, 0), logsums)


def attention_backward(query, keys, values, mixed_all, logsums, grad_mixed, between):
    length = query.shape[0]
    factor = HD ** (-0.5)
    grad_query, key_total, value_total = [], None, None
    for (start, stop), logsum in reversed(list(zip(blocks_of(length), logsums))):
        query_block = query[start:stop]
        grad_block = grad_mixed[start:stop]
        mixed_block = mixed_all[start:stop]
        scores = scores_block(query_block, keys[:stop], start)
        chances = jnp.exp(scores - logsum)
        weights_low = chances.astype(jnp.bfloat16)
        delta = jnp.sum(grad_block.astype(jnp.float32) * mixed_block.astype(jnp.float32), axis=-1)
        grad_weights = jnp.einsum(
            "qhd,khd->hqk", grad_block, values[:stop], preferred_element_type=jnp.float32
        )
        grad_scores = (chances * (grad_weights - delta.T[:, :, None])).astype(jnp.bfloat16)
        grad_query.append(
            jnp.einsum(
                "hqk,khd->qhd", grad_scores, keys[:stop], preferred_element_type=jnp.float32
            )
            * factor
        )
        key_part = (
            jnp.einsum("hqk,qhd->khd", grad_scores, query_block, preferred_element_type=jnp.float32)
            * factor
        )
        value_part = jnp.einsum(
            "hqk,qhd->khd", weights_low, grad_block, preferred_element_type=jnp.float32
        )
        if key_total is None:
            key_total, value_total = key_part, value_part
            grad_mixed, key_total = between((grad_mixed, key_total))
        else:
            key_total = key_total.at[:stop].add(key_part)
            value_total = value_total.at[:stop].add(value_part)
    return (jnp.concatenate(grad_query[::-1], 0), key_total, value_total)


def gather_rows(array):
    return lax.all_gather(array, "fsdp", axis=0, tiled=True)


def product_nt(inputs, weight):
    return lax.dot_general(
        inputs, weight, (((1,), (1,)), ((), ())), preferred_element_type=jnp.float32
    )


def product_tn(left, right):
    return lax.dot_general(
        left, right, (((0,), (0,)), ((), ())), preferred_element_type=jnp.float32
    )


def scatter_sum(partial):
    return lax.psum_scatter(
        partial.astype(jnp.bfloat16), "fsdp", scatter_dimension=0, tiled=True
    ).astype(jnp.float32)


class Chain:
    def __init__(self, partial, count):
        half = count // 2
        self.count = count
        self.value = partial.astype(jnp.bfloat16)
        self.flying = None
        self.hops = []
        if count % 2 == 0:
            for s in range(half - 1):
                self.hops.append(([(s, s + 1), (count - 1 - s, count - 2 - s)], None))
            self.hops.append(([(half - 1, half), (half, half - 1)], None))
            for s in reversed(range(half - 1)):
                self.hops.append(([(s + 1, s), (count - 2 - s, count - 1 - s)], s))
        elif count > 1:
            self.value = lax.psum(self.value, "sp")
        self.at = 0

    def send(self):
        if self.at < len(self.hops):
            self.flying = lax.ppermute(self.value, "sp", self.hops[self.at][0])

    def take(self):
        depth = self.hops[self.at][1]
        if depth is None:
            total = self.value.astype(jnp.float32) + self.flying.astype(jnp.float32)
            self.value = total.astype(jnp.bfloat16)
        else:
            place = lax.axis_index("sp")
            mine = jnp.minimum(place, self.count - 1 - place) == depth
            self.value = jnp.where(mine, self.flying, self.value)
        self.at += 1
        self.flying = None

    def finish(self):
        while self.at < len(self.hops):
            if self.flying is None:
                self.send()
            self.take()
        return self.value


def meet(values, moving, starting=()):
    moving = [c for c in moving if c.flying is not None]
    tied = lax.optimization_barrier(
        (values, [c.flying for c in moving], [c.value for c in starting])
    )
    for chain, arrived in zip(moving, tied[1]):
        chain.flying = arrived
        chain.take()
        chain.send()
    for chain, value in zip(starting, tied[2]):
        chain.value = value
        chain.send()
    return tied[0]


def turn(blocks, ways):
    me = lax.axis_index("fsdp")
    result = lax.dynamic_update_slice_in_dim(
        jnp.zeros_like(blocks), lax.dynamic_slice_in_dim(blocks, me, 1, 0), me, 0
    )
    for shift in range(1, ways):
        block = lax.dynamic_slice_in_dim(blocks, (me + shift) % ways, 1, 0)
        pairs = [(f, (f + shift) % ways) for f in range(ways)]
        arrived = lax.ppermute(block, "fsdp", pairs)
        result = lax.dynamic_update_slice_in_dim(result, arrived, (me - shift) % ways, 0)
    return result


def sum_all(values, sizes):
    for axis, size in sizes:
        if size & (size - 1):
            values = lax.psum(values, axis)
            continue
        step = 1
        while step < size:
            values = values + lax.ppermute(values, axis, [(d, d ^ step) for d in range(size)])
            step *= 2
    return values


def halves(array):
    middle = array.shape[0] // 2
    return (array[:middle], array[middle:])


def layer(
    ways,
    line,
    hidden_in,
    positions,
    attn_gain,
    qkv_weight,
    query_gain,
    key_gain,
    out_weight,
    mlp_gain,
    gate_up_weight,
    down_weight,
    cotangent,
):
    f32 = jnp.float32
    low = jnp.bfloat16
    rows, width = hidden_in.shape
    group = H // KV
    units = FF // ways
    pairs_of = ways // 2
    side = lax.axis_index("fsdp") // pairs_of
    swap = [(f, (f + pairs_of) % ways) for f in range(ways)]

    qkv_full = gather_rows(qkv_weight)
    qkv_full, gate_up_late, down_late, out_late, cotangent_late = lax.optimization_barrier(
        (qkv_full, gate_up_weight, down_weight, out_weight, cotangent)
    )
    out_full = gather_rows(out_late)
    cotangent_all = gather_rows(cotangent_late)
    kept = lax.dynamic_slice_in_dim(gate_up_late, side * units, units, 0)
    sent = lax.dynamic_slice_in_dim(gate_up_late, (1 - side) * units, units, 0)
    swapped = lax.ppermute(sent, "fsdp", swap)
    gate_up_own = jnp.concatenate([kept, swapped], 0)
    down_split = down_late.reshape(-1, pairs_of, 2, units).transpose(2, 1, 0, 3)
    down_own = turn(down_split.reshape(ways, -1, units), ways).reshape(width, units)
    hidden = hidden_in.astype(f32)
    normed1, inverse1 = rms_forward(hidden, attn_gain)
    normed1_low = normed1.astype(low)
    projected = product_nt(normed1_low, qkv_full)
    query = projected[:, : H * HD].reshape(rows, H, HD)
    key = projected[:, H * HD : (H + KV) * HD].reshape(rows, KV, HD)
    value_low = projected[:, (H + KV) * HD :].astype(low)
    cosine, sine = rotary_tables(positions)
    query_normed, query_inverse = rms_forward(query, query_gain)
    key_normed, key_inverse = rms_forward(key, key_gain)
    query_low = rotate(query_normed, cosine, sine).astype(low).reshape(rows, H * HD)
    key_low = rotate(key_normed, cosine, sine).astype(low).reshape(rows, KV * HD)
    query_heads, key_heads, value_heads = (
        lax.all_to_all(query_low, "sp", split_axis=1, concat_axis=0, tiled=True),
        lax.all_to_all(key_low, "sp", split_axis=1, concat_axis=0, tiled=True),
        lax.all_to_all(value_low, "sp", split_axis=1, concat_axis=0, tiled=True),
    )
    length = query_heads.shape[0]
    local_kv = key_heads.shape[1] // HD
    query_local = query_heads.reshape(length, -1, HD)
    keys_local = jnp.repeat(key_heads.reshape(length, local_kv, HD), group, axis=1)
    values_local = jnp.repeat(value_heads.reshape(length, local_kv, HD), group, axis=1)
    mixed_heads, logsums = attention_forward(query_local, keys_local, values_local)
    attended = lax.all_to_all(
        mixed_heads.reshape(length, -1), "sp", split_axis=0, concat_axis=1, tiled=True
    )
    middle = hidden + product_nt(attended, out_full)
    normed2, inverse2 = rms_forward(middle, mlp_gain)
    normed2_all = gather_rows(normed2.astype(low))
    normed1_late, middle = lax.optimization_barrier((normed1_low, middle))
    normed1_all = gather_rows(normed1_late)

    grad_act = jnp.dot(cotangent_all, down_own, preferred_element_type=f32)
    both = product_nt(normed2_all, gate_up_own)
    first, second = both[:, :units], both[:, units:]
    gate = jnp.where(side == 0, first, second)
    upper = jnp.where(side == 0, second, first)
    sigmoid = jax.nn.sigmoid(gate)
    activation = (gate * sigmoid * upper).astype(low)
    grad_gate = grad_act * upper * sigmoid * (1.0 + gate * (1.0 - sigmoid))
    grad_upper = grad_act * gate * sigmoid
    grad_first = jnp.where(side == 0, grad_gate, grad_upper).astype(low)
    grad_second = jnp.where(side == 0, grad_upper, grad_gate).astype(low)
    grad_both = jnp.concatenate([grad_first, grad_second], 1)
    grad_normed2 = scatter_sum(jnp.dot(grad_both, gate_up_own, preferred_element_type=f32))
    grad_sent = product_tn(grad_second, normed2_all).astype(low)
    s0, s1 = (Chain(part, line) for part in halves(grad_sent))
    s0.send()
    s1.send()
    grad_down_own = product_tn(cotangent_all, activation).astype(low)
    grad_kept = product_tn(grad_first, normed2_all).astype(low)
    grad_kept, grad_down_own = meet((grad_kept, grad_down_own), [s0])
    d0, d1 = (Chain(part, line) for part in halves(grad_down_own))
    k0, k1 = (Chain(part, line) for part in halves(grad_kept))

    back_two, mlp_term = rms_backward(middle, inverse2, mlp_gain, grad_normed2)
    grad_middle = cotangent.astype(f32) + back_two
    grad_mixed_low = grad_middle.astype(low)
    grad_attended = jnp.dot(grad_mixed_low, out_full, preferred_element_type=f32).astype(low)
    grad_heads = lax.all_to_all(grad_attended, "sp", split_axis=1, concat_axis=0, tiled=True)
    grad_mixed_low = meet(grad_mixed_low, [s1], [d0, d1])
    grad_out = scatter_sum(product_tn(grad_mixed_low, attended))
    grad_query_local, grad_keys, grad_values = attention_backward(
        query_local,
        keys_local,
        values_local,
        mixed_heads,
        logsums,
        grad_heads.reshape(length, -1, HD),
        lambda values: meet(values, [s0]),
    )
    grad_query_send = grad_query_local.astype(low).reshape(length, -1)
    grad_key_send = (
        grad_keys.reshape(length, local_kv, group, HD).sum(2).astype(low).reshape(length, -1)
    )
    grad_value_send = (
        grad_values.reshape(length, local_kv, group, HD).sum(2).astype(low).reshape(length, -1)
    )
    grads_send = jnp.concatenate([grad_query_send, grad_key_send, grad_value_send], 1)
    grads_send, activation = meet((grads_send, activation), [s1, d0])
    grads_low = lax.all_to_all(grads_send, "sp", split_axis=0, concat_axis=1, tiled=True)
    hidden_out = (middle + scatter_sum(product_nt(activation, down_own))).astype(low)
    grads_low = meet(grads_low, [d1], [k0, k1])
    grads_low = grads_low.reshape(rows, line, -1)
    cuts = (grad_query_send.shape[1], grad_query_send.shape[1] + grad_key_send.shape[1])
    grad_query_low = grads_low[:, :, : cuts[0]]
    grad_key_low = grads_low[:, :, cuts[0] : cuts[1]]
    grad_value_low = grads_low[:, :, cuts[1] :].reshape(rows, KV * HD)
    grad_query, query_term = rms_backward(
        query,
        query_inverse,
        query_gain,
        rotate_back(grad_query_low.astype(f32).reshape(rows, H, HD), cosine, sine),
    )
    grad_query, query_term = meet((grad_query, query_term), [d0, k0])
    grad_key, key_term = rms_backward(
        key,
        key_inverse,
        key_gain,
        rotate_back(grad_key_low.astype(f32).reshape(rows, KV, HD), cosine, sine),
    )
    grad_projected = jnp.concatenate(
        [
            grad_query.reshape(rows, H * HD).astype(low),
            grad_key.reshape(rows, KV * HD).astype(low),
            grad_value_low,
        ],
        1,
    )
    grad_columns = lax.all_to_all(grad_projected, "fsdp", split_axis=1, concat_axis=0, tiled=True)
    out_chain = Chain(grad_out, line)
    grad_columns = meet(grad_columns, [d1, k1, s0, s1], [out_chain])
    swapped_back = []
    for chain in (s0, s1):
        swapped_back.append(lax.ppermute(chain.finish(), "fsdp", swap))
    grad_normed1 = jnp.dot(grad_projected, qkv_full, preferred_element_type=f32)
    grad_qkv_own = product_tn(grad_columns, normed1_all).astype(low)
    back_one, attn_term = rms_backward(hidden, inverse1, attn_gain, grad_normed1)
    grad_input = grad_middle + back_one
    terms = jnp.concatenate(
        [
            jnp.sum(attn_term, axis=0),
            jnp.sum(mlp_term, axis=0),
            jnp.sum(query_term, axis=(0, 1)),
            jnp.sum(key_term, axis=(0, 1)),
        ]
    )
    grad_qkv_own, terms = meet((grad_qkv_own, terms), [k0])
    q0, q1 = (Chain(part, line) for part in halves(grad_qkv_own))
    q0.send()
    q1.send()
    meet((), [out_chain])
    swapped_back = [meet(swapped_back[0], [q0]), meet(swapped_back[1], [q1])]
    sums = sum_all(terms, (("fsdp", ways), ("sp", line)))
    grad_swapped = jnp.concatenate(swapped_back, 0)
    grad_down_sum = jnp.concatenate([d0.finish(), d1.finish()], 0)
    down_back = lax.all_to_all(
        grad_down_sum.reshape(ways, -1, units),
        "fsdp",
        split_axis=0,
        concat_axis=0,
        tiled=True,
    )
    grad_down = (
        down_back.reshape(2, pairs_of, -1, units)
        .transpose(2, 1, 0, 3)
        .reshape(down_weight.shape)
        .astype(f32)
    )
    grad_kept = jnp.concatenate([k0.finish(), k1.finish()], 0)
    grad_gate_up = jnp.concatenate(
        [
            jnp.where(side == 0, grad_kept, grad_swapped),
            jnp.where(side == 0, grad_swapped, grad_kept),
        ],
        0,
    ).astype(f32)
    grad_out = out_chain.finish().astype(f32)
    grad_qkv = jnp.concatenate([q0.finish(), q1.finish()], 0).astype(f32)
    gains = (
        sums[:width],
        sums[2 * width : 2 * width + HD],
        sums[2 * width + HD :],
        sums[width : 2 * width],
    )
    return (
        hidden_out,
        grad_input,
        gains[0],
        grad_qkv,
        gains[1],
        gains[2],
        grad_out,
        gains[3],
        grad_gate_up,
        grad_down,
    )


def solution(mesh):
    return jax.shard_map(
        functools.partial(layer, mesh.shape["fsdp"], mesh.shape["sp"]),
        mesh=mesh,
        in_specs=(
            P(("fsdp", "sp"), None),
            P(("fsdp", "sp")),
            P(),
            P("fsdp", None),
            P(),
            P(),
            P("fsdp", None),
            P(),
            P("fsdp", None),
            P("fsdp", None),
            P(("fsdp", "sp"), None),
        ),
        out_specs=(
            P(("fsdp", "sp"), None),
            P(("fsdp", "sp"), None),
            P(),
            P("fsdp", None),
            P(),
            P(),
            P("fsdp", None),
            P(),
            P("fsdp", None),
            P("fsdp", None),
        ),
        check_vma=False,
    )
```

```python
import functools

import jax
import jax.numpy as jnp
from jax import lax
from jax.sharding import PartitionSpec as P


H = 16
KV = 8
HD = 128
FF = 6144


EPS = 1e-06
THETA = 1000000.0
NEGATIVE = -1e30


def rms_forward(values, gain):
    inverse = lax.rsqrt(jnp.mean(values * values, axis=-1, keepdims=True) + EPS)
    return (values * inverse * gain, inverse)


def rms_backward(values, inverse, gain, upstream):
    scaled = upstream * gain
    cubed = inverse * inverse * inverse
    gradient = inverse * scaled - values * cubed * jnp.mean(scaled * values, axis=-1, keepdims=True)
    return (gradient, upstream * values * inverse)


def rotary_tables(positions):
    half = HD // 2
    frequency = THETA ** (-(jnp.arange(half, dtype=jnp.float32) * 2.0 / HD))
    angle = positions.astype(jnp.float32)[:, None] * frequency[None, :]
    cosine = jnp.cos(angle)
    sine = jnp.sin(angle)
    return (
        jnp.concatenate([cosine, cosine], -1)[:, None, :],
        jnp.concatenate([sine, sine], -1)[:, None, :],
    )


def rotate(values, cosine, sine):
    half = HD // 2
    turned = jnp.concatenate([-values[..., half:], values[..., :half]], -1)
    return values * cosine + turned * sine


def rotate_back(gradient, cosine, sine):
    half = HD // 2
    scaled = gradient * sine
    return gradient * cosine + jnp.concatenate([scaled[..., half:], -scaled[..., :half]], -1)


def scores_block(query_block, keys, start):
    scores = jnp.einsum("qhd,khd->hqk", query_block, keys, preferred_element_type=jnp.float32)
    query_rows = start + jnp.arange(query_block.shape[0])
    key_rows = jnp.arange(keys.shape[0])
    allowed = key_rows[None, :] <= query_rows[:, None]
    return jnp.where(allowed[None], scores * HD ** (-0.5), NEGATIVE)


def blocks_of(length):
    block = min(512, length)
    return [(start, start + block) for start in range(0, length, block)]


def attention_forward(query, keys, values):
    mixed_all, logsums = [], []
    for start, stop in blocks_of(query.shape[0]):
        scores = scores_block(query[start:stop], keys[:stop], start)
        top = jnp.max(scores, axis=-1, keepdims=True)
        logsum = top + jnp.log(jnp.sum(jnp.exp(scores - top), axis=-1, keepdims=True))
        weights = jnp.exp(scores - logsum).astype(jnp.bfloat16)
        mixed = jnp.einsum(
            "hqk,khd->qhd", weights, values[:stop], preferred_element_type=jnp.float32
        )
        mixed_all.append(mixed.astype(jnp.bfloat16))
        logsums.append(logsum)
    return (jnp.concatenate(mixed_all, 0), logsums)


def attention_backward(query, keys, values, mixed_all, logsums, grad_mixed, between):
    length = query.shape[0]
    factor = HD ** (-0.5)
    grad_query, key_total, value_total = [], None, None
    for (start, stop), logsum in reversed(list(zip(blocks_of(length), logsums))):
        query_block = query[start:stop]
        grad_block = grad_mixed[start:stop]
        mixed_block = mixed_all[start:stop]
        scores = scores_block(query_block, keys[:stop], start)
        chances = jnp.exp(scores - logsum)
        weights_low = chances.astype(jnp.bfloat16)
        delta = jnp.sum(grad_block.astype(jnp.float32) * mixed_block.astype(jnp.float32), axis=-1)
        grad_weights = jnp.einsum(
            "qhd,khd->hqk", grad_block, values[:stop], preferred_element_type=jnp.float32
        )
        grad_scores = (chances * (grad_weights - delta.T[:, :, None])).astype(jnp.bfloat16)
        grad_query.append(
            jnp.einsum(
                "hqk,khd->qhd", grad_scores, keys[:stop], preferred_element_type=jnp.float32
            )
            * factor
        )
        key_part = (
            jnp.einsum("hqk,qhd->khd", grad_scores, query_block, preferred_element_type=jnp.float32)
            * factor
        )
        value_part = jnp.einsum(
            "hqk,qhd->khd", weights_low, grad_block, preferred_element_type=jnp.float32
        )
        if key_total is None:
            key_total, value_total = key_part, value_part
            grad_mixed, key_total = between((grad_mixed, key_total))
        else:
            key_total = key_total.at[:stop].add(key_part)
            value_total = value_total.at[:stop].add(value_part)
    return (jnp.concatenate(grad_query[::-1], 0), key_total, value_total)


def gather_rows(array):
    return lax.all_gather(array, "fsdp", axis=0, tiled=True)


def product_nt(inputs, weight):
    return lax.dot_general(
        inputs, weight, (((1,), (1,)), ((), ())), preferred_element_type=jnp.float32
    )


def product_tn(left, right):
    return lax.dot_general(
        left, right, (((0,), (0,)), ((), ())), preferred_element_type=jnp.float32
    )


def scatter_sum(partial):
    return lax.psum_scatter(
        partial.astype(jnp.bfloat16), "fsdp", scatter_dimension=0, tiled=True
    ).astype(jnp.float32)


class Chain:
    def __init__(self, partial, count):
        half = count // 2
        self.count = count
        self.value = partial.astype(jnp.bfloat16)
        self.flying = None
        self.hops = []
        if count % 2 == 0:
            for s in range(half - 1):
                self.hops.append(([(s, s + 1), (count - 1 - s, count - 2 - s)], None))
            self.hops.append(([(half - 1, half), (half, half - 1)], None))
            for s in reversed(range(half - 1)):
                self.hops.append(([(s + 1, s), (count - 2 - s, count - 1 - s)], s))
        elif count > 1:
            self.value = lax.psum(self.value, "sp")
        self.at = 0

    def send(self):
        if self.at < len(self.hops):
            self.flying = lax.ppermute(self.value, "sp", self.hops[self.at][0])

    def take(self):
        depth = self.hops[self.at][1]
        if depth is None:
            total = self.value.astype(jnp.float32) + self.flying.astype(jnp.float32)
            self.value = total.astype(jnp.bfloat16)
        else:
            place = lax.axis_index("sp")
            mine = jnp.minimum(place, self.count - 1 - place) == depth
            self.value = jnp.where(mine, self.flying, self.value)
        self.at += 1
        self.flying = None

    def finish(self):
        while self.at < len(self.hops):
            if self.flying is None:
                self.send()
            self.take()
        return self.value


def meet(values, moving, starting=()):
    moving = [c for c in moving if c.flying is not None]
    tied = lax.optimization_barrier(
        (values, [c.flying for c in moving], [c.value for c in starting])
    )
    for chain, arrived in zip(moving, tied[1]):
        chain.flying = arrived
        chain.take()
        chain.send()
    for chain, value in zip(starting, tied[2]):
        chain.value = value
        chain.send()
    return tied[0]


def turn(blocks, ways):
    me = lax.axis_index("fsdp")
    result = lax.dynamic_update_slice_in_dim(
        jnp.zeros_like(blocks), lax.dynamic_slice_in_dim(blocks, me, 1, 0), me, 0
    )
    for shift in range(1, ways):
        block = lax.dynamic_slice_in_dim(blocks, (me + shift) % ways, 1, 0)
        pairs = [(f, (f + shift) % ways) for f in range(ways)]
        arrived = lax.ppermute(block, "fsdp", pairs)
        result = lax.dynamic_update_slice_in_dim(result, arrived, (me - shift) % ways, 0)
    return result


def sum_all(values, sizes):
    for axis, size in sizes:
        if size & (size - 1):
            values = lax.psum(values, axis)
            continue
        step = 1
        while step < size:
            values = values + lax.ppermute(values, axis, [(d, d ^ step) for d in range(size)])
            step *= 2
    return values


def halves(array):
    middle = array.shape[0] // 2
    return (array[:middle], array[middle:])


def layer(
    ways,
    line,
    hidden_in,
    positions,
    attn_gain,
    qkv_weight,
    query_gain,
    key_gain,
    out_weight,
    mlp_gain,
    gate_up_weight,
    down_weight,
    cotangent,
):
    f32 = jnp.float32
    low = jnp.bfloat16
    rows, width = hidden_in.shape
    group = H // KV
    units = FF // ways
    pairs_of = ways // 2
    side = lax.axis_index("fsdp") // pairs_of
    swap = [(f, (f + pairs_of) % ways) for f in range(ways)]

    qkv_full = gather_rows(qkv_weight)
    qkv_full, gate_up_late, down_late, out_late, cotangent_late = lax.optimization_barrier(
        (qkv_full, gate_up_weight, down_weight, out_weight, cotangent)
    )
    out_full = gather_rows(out_late)
    cotangent_all = gather_rows(cotangent_late)
    kept = lax.dynamic_slice_in_dim(gate_up_late, side * units, units, 0)
    sent = lax.dynamic_slice_in_dim(gate_up_late, (1 - side) * units, units, 0)
    swapped = lax.ppermute(sent, "fsdp", swap)
    gate_up_own = jnp.concatenate([kept, swapped], 0)
    down_split = down_late.reshape(-1, pairs_of, 2, units).transpose(2, 1, 0, 3)
    down_own = turn(down_split.reshape(ways, -1, units), ways).reshape(width, units)
    hidden = hidden_in.astype(f32)
    normed1, inverse1 = rms_forward(hidden, attn_gain)
    normed1_low = normed1.astype(low)
    projected = product_nt(normed1_low, qkv_full)
    query = projected[:, : H * HD].reshape(rows, H, HD)
    key = projected[:, H * HD : (H + KV) * HD].reshape(rows, KV, HD)
    value_low = projected[:, (H + KV) * HD :].astype(low)
    cosine, sine = rotary_tables(positions)
    query_normed, query_inverse = rms_forward(query, query_gain)
    key_normed, key_inverse = rms_forward(key, key_gain)
    query_low = rotate(query_normed, cosine, sine).astype(low).reshape(rows, H * HD)
    key_low = rotate(key_normed, cosine, sine).astype(low).reshape(rows, KV * HD)
    query_heads, key_heads, value_heads = (
        lax.all_to_all(query_low, "sp", split_axis=1, concat_axis=0, tiled=True),
        lax.all_to_all(key_low, "sp", split_axis=1, concat_axis=0, tiled=True),
        lax.all_to_all(value_low, "sp", split_axis=1, concat_axis=0, tiled=True),
    )
    length = query_heads.shape[0]
    local_kv = key_heads.shape[1] // HD
    query_local = query_heads.reshape(length, -1, HD)
    keys_local = jnp.repeat(key_heads.reshape(length, local_kv, HD), group, axis=1)
    values_local = jnp.repeat(value_heads.reshape(length, local_kv, HD), group, axis=1)
    mixed_heads, logsums = attention_forward(query_local, keys_local, values_local)
    attended = lax.all_to_all(
        mixed_heads.reshape(length, -1), "sp", split_axis=0, concat_axis=1, tiled=True
    )
    middle = hidden + product_nt(attended, out_full)
    normed2, inverse2 = rms_forward(middle, mlp_gain)
    normed2_all = gather_rows(normed2.astype(low))
    normed1_late, middle = lax.optimization_barrier((normed1_low, middle))
    normed1_all = gather_rows(normed1_late)

    grad_act = jnp.dot(cotangent_all, down_own, preferred_element_type=f32)
    both = product_nt(normed2_all, gate_up_own)
    first, second = both[:, :units], both[:, units:]
    gate = jnp.where(side == 0, first, second)
    upper = jnp.where(side == 0, second, first)
    sigmoid = jax.nn.sigmoid(gate)
    activation = (gate * sigmoid * upper).astype(low)
    grad_gate = grad_act * upper * sigmoid * (1.0 + gate * (1.0 - sigmoid))
    grad_upper = grad_act * gate * sigmoid
    grad_first = jnp.where(side == 0, grad_gate, grad_upper).astype(low)
    grad_second = jnp.where(side == 0, grad_upper, grad_gate).astype(low)
    grad_both = jnp.concatenate([grad_first, grad_second], 1)
    grad_normed2 = scatter_sum(jnp.dot(grad_both, gate_up_own, preferred_element_type=f32))
    grad_sent = product_tn(grad_second, normed2_all).astype(low)
    s0, s1 = (Chain(part, line) for part in halves(grad_sent))
    s0.send()
    s1.send()
    grad_down_own = product_tn(cotangent_all, activation).astype(low)
    grad_kept = product_tn(grad_first, normed2_all).astype(low)
    grad_kept, grad_down_own = meet((grad_kept, grad_down_own), [s0])
    d0, d1 = (Chain(part, line) for part in halves(grad_down_own))
    k0, k1 = (Chain(part, line) for part in halves(grad_kept))

    back_two, mlp_term = rms_backward(middle, inverse2, mlp_gain, grad_normed2)
    grad_middle = cotangent.astype(f32) + back_two
    grad_mixed_low = grad_middle.astype(low)
    grad_attended = jnp.dot(grad_mixed_low, out_full, preferred_element_type=f32).astype(low)
    grad_heads = lax.all_to_all(grad_attended, "sp", split_axis=1, concat_axis=0, tiled=True)
    grad_mixed_low = meet(grad_mixed_low, [s1], [d0, d1])
    grad_out = scatter_sum(product_tn(grad_mixed_low, attended))
    grad_query_local, grad_keys, grad_values = attention_backward(
        query_local,
        keys_local,
        values_local,
        mixed_heads,
        logsums,
        grad_heads.reshape(length, -1, HD),
        lambda values: meet(values, [s0]),
    )
    grad_query_send = grad_query_local.astype(low).reshape(length, -1)
    grad_key_send = (
        grad_keys.reshape(length, local_kv, group, HD).sum(2).astype(low).reshape(length, -1)
    )
    grad_value_send = (
        grad_values.reshape(length, local_kv, group, HD).sum(2).astype(low).reshape(length, -1)
    )
    grads_send = jnp.concatenate([grad_query_send, grad_key_send, grad_value_send], 1)
    grads_send, activation = meet((grads_send, activation), [s1, d0], [k0, k1])
    grads_low = lax.all_to_all(grads_send, "sp", split_axis=0, concat_axis=1, tiled=True)
    hidden_out = (middle + scatter_sum(product_nt(activation, down_own))).astype(low)
    grads_low = meet(grads_low, [d1])
    grads_low = grads_low.reshape(rows, line, -1)
    cuts = (grad_query_send.shape[1], grad_query_send.shape[1] + grad_key_send.shape[1])
    grad_query_low = grads_low[:, :, : cuts[0]]
    grad_key_low = grads_low[:, :, cuts[0] : cuts[1]]
    grad_value_low = grads_low[:, :, cuts[1] :].reshape(rows, KV * HD)
    grad_query, query_term = rms_backward(
        query,
        query_inverse,
        query_gain,
        rotate_back(grad_query_low.astype(f32).reshape(rows, H, HD), cosine, sine),
    )
    grad_query, query_term = meet((grad_query, query_term), [d0, k0])
    grad_key, key_term = rms_backward(
        key,
        key_inverse,
        key_gain,
        rotate_back(grad_key_low.astype(f32).reshape(rows, KV, HD), cosine, sine),
    )
    grad_projected = jnp.concatenate(
        [
            grad_query.reshape(rows, H * HD).astype(low),
            grad_key.reshape(rows, KV * HD).astype(low),
            grad_value_low,
        ],
        1,
    )
    grad_columns = lax.all_to_all(grad_projected, "fsdp", split_axis=1, concat_axis=0, tiled=True)
    out_chain = Chain(grad_out, line)
    grad_columns = meet(grad_columns, [d1, k0, k1, s0, s1], [out_chain])
    swapped_back = []
    for chain in (s0, s1):
        swapped_back.append(lax.ppermute(chain.finish(), "fsdp", swap))
    grad_normed1 = jnp.dot(grad_projected, qkv_full, preferred_element_type=f32)
    grad_qkv_own = product_tn(grad_columns, normed1_all).astype(low)
    back_one, attn_term = rms_backward(hidden, inverse1, attn_gain, grad_normed1)
    grad_input = grad_middle + back_one
    terms = jnp.concatenate(
        [
            jnp.sum(attn_term, axis=0),
            jnp.sum(mlp_term, axis=0),
            jnp.sum(query_term, axis=(0, 1)),
            jnp.sum(key_term, axis=(0, 1)),
        ]
    )
    grad_qkv_own, terms = meet((grad_qkv_own, terms), [])
    q0, q1 = (Chain(part, line) for part in halves(grad_qkv_own))
    q0.send()
    q1.send()
    meet((), [out_chain])
    meet((), [k1])
    swapped_back = [meet(swapped_back[0], [q0]), meet(swapped_back[1], [q1])]
    grad_swapped = jnp.concatenate(swapped_back, 0)
    grad_down_sum = jnp.concatenate([d0.finish(), d1.finish()], 0)
    down_back = lax.all_to_all(
        grad_down_sum.reshape(ways, -1, units),
        "fsdp",
        split_axis=0,
        concat_axis=0,
        tiled=True,
    )
    down_back, terms = meet((down_back, terms), [])
    sums = sum_all(terms, (("fsdp", ways), ("sp", line)))
    grad_down = (
        down_back.reshape(2, pairs_of, -1, units)
        .transpose(2, 1, 0, 3)
        .reshape(down_weight.shape)
        .astype(f32)
    )
    grad_kept = jnp.concatenate([k0.finish(), k1.finish()], 0)
    grad_gate_up = jnp.concatenate(
        [
            jnp.where(side == 0, grad_kept, grad_swapped),
            jnp.where(side == 0, grad_swapped, grad_kept),
        ],
        0,
    ).astype(f32)
    grad_out = out_chain.finish().astype(f32)
    grad_qkv = jnp.concatenate([q0.finish(), q1.finish()], 0).astype(f32)
    gains = (
        sums[:width],
        sums[2 * width : 2 * width + HD],
        sums[2 * width + HD :],
        sums[width : 2 * width],
    )
    return (
        hidden_out,
        grad_input,
        gains[0],
        grad_qkv,
        gains[1],
        gains[2],
        grad_out,
        gains[3],
        grad_gate_up,
        grad_down,
    )


def solution(mesh):
    return jax.shard_map(
        functools.partial(layer, mesh.shape["fsdp"], mesh.shape["sp"]),
        mesh=mesh,
        in_specs=(
            P(("fsdp", "sp"), None),
            P(("fsdp", "sp")),
            P(),
            P("fsdp", None),
            P(),
            P(),
            P("fsdp", None),
            P(),
            P("fsdp", None),
            P("fsdp", None),
            P(("fsdp", "sp"), None),
        ),
        out_specs=(
            P(("fsdp", "sp"), None),
            P(("fsdp", "sp"), None),
            P(),
            P("fsdp", None),
            P(),
            P(),
            P("fsdp", None),
            P(),
            P("fsdp", None),
            P("fsdp", None),
        ),
        check_vma=False,
    )
```

```python
import functools

import jax
import jax.numpy as jnp
from jax import lax
from jax.sharding import PartitionSpec as P


H = 16
KV = 8
HD = 128
FF = 6144


EPS = 1e-06
THETA = 1000000.0
NEGATIVE = -1e30


def rms_forward(values, gain):
    inverse = lax.rsqrt(jnp.mean(values * values, axis=-1, keepdims=True) + EPS)
    return (values * inverse * gain, inverse)


def rms_backward(values, inverse, gain, upstream):
    scaled = upstream * gain
    cubed = inverse * inverse * inverse
    gradient = inverse * scaled - values * cubed * jnp.mean(scaled * values, axis=-1, keepdims=True)
    return (gradient, upstream * values * inverse)


def rotary_tables(positions):
    half = HD // 2
    frequency = THETA ** (-(jnp.arange(half, dtype=jnp.float32) * 2.0 / HD))
    angle = positions.astype(jnp.float32)[:, None] * frequency[None, :]
    cosine = jnp.cos(angle)
    sine = jnp.sin(angle)
    return (
        jnp.concatenate([cosine, cosine], -1)[:, None, :],
        jnp.concatenate([sine, sine], -1)[:, None, :],
    )


def rotate(values, cosine, sine):
    half = HD // 2
    turned = jnp.concatenate([-values[..., half:], values[..., :half]], -1)
    return values * cosine + turned * sine


def rotate_back(gradient, cosine, sine):
    half = HD // 2
    scaled = gradient * sine
    return gradient * cosine + jnp.concatenate([scaled[..., half:], -scaled[..., :half]], -1)


def scores_block(query_block, keys, start):
    scores = jnp.einsum("qhd,khd->hqk", query_block, keys, preferred_element_type=jnp.float32)
    query_rows = start + jnp.arange(query_block.shape[0])
    key_rows = jnp.arange(keys.shape[0])
    allowed = key_rows[None, :] <= query_rows[:, None]
    return jnp.where(allowed[None], scores * HD ** (-0.5), NEGATIVE)


def blocks_of(length):
    block = min(512, length)
    return [(start, start + block) for start in range(0, length, block)]


def attention_forward(query, keys, values):
    mixed_all, logsums = [], []
    for start, stop in blocks_of(query.shape[0]):
        scores = scores_block(query[start:stop], keys[:stop], start)
        top = jnp.max(scores, axis=-1, keepdims=True)
        logsum = top + jnp.log(jnp.sum(jnp.exp(scores - top), axis=-1, keepdims=True))
        weights = jnp.exp(scores - logsum).astype(jnp.bfloat16)
        mixed = jnp.einsum(
            "hqk,khd->qhd", weights, values[:stop], preferred_element_type=jnp.float32
        )
        mixed_all.append(mixed.astype(jnp.bfloat16))
        logsums.append(logsum)
    return (jnp.concatenate(mixed_all, 0), logsums)


def attention_backward(query, keys, values, mixed_all, logsums, grad_mixed, between):
    length = query.shape[0]
    factor = HD ** (-0.5)
    grad_query, key_total, value_total = [], None, None
    for (start, stop), logsum in reversed(list(zip(blocks_of(length), logsums))):
        query_block = query[start:stop]
        grad_block = grad_mixed[start:stop]
        mixed_block = mixed_all[start:stop]
        scores = scores_block(query_block, keys[:stop], start)
        chances = jnp.exp(scores - logsum)
        weights_low = chances.astype(jnp.bfloat16)
        delta = jnp.sum(grad_block.astype(jnp.float32) * mixed_block.astype(jnp.float32), axis=-1)
        grad_weights = jnp.einsum(
            "qhd,khd->hqk", grad_block, values[:stop], preferred_element_type=jnp.float32
        )
        grad_scores = (chances * (grad_weights - delta.T[:, :, None])).astype(jnp.bfloat16)
        grad_query.append(
            jnp.einsum(
                "hqk,khd->qhd", grad_scores, keys[:stop], preferred_element_type=jnp.float32
            )
            * factor
        )
        key_part = (
            jnp.einsum("hqk,qhd->khd", grad_scores, query_block, preferred_element_type=jnp.float32)
            * factor
        )
        value_part = jnp.einsum(
            "hqk,qhd->khd", weights_low, grad_block, preferred_element_type=jnp.float32
        )
        if key_total is None:
            key_total, value_total = key_part, value_part
            grad_mixed, key_total = between((grad_mixed, key_total))
        else:
            key_total = key_total.at[:stop].add(key_part)
            value_total = value_total.at[:stop].add(value_part)
    return (jnp.concatenate(grad_query[::-1], 0), key_total, value_total)


def gather_rows(array):
    return lax.all_gather(array, "fsdp", axis=0, tiled=True)


def product_nt(inputs, weight):
    return lax.dot_general(
        inputs, weight, (((1,), (1,)), ((), ())), preferred_element_type=jnp.float32
    )


def product_tn(left, right):
    return lax.dot_general(
        left, right, (((0,), (0,)), ((), ())), preferred_element_type=jnp.float32
    )


def scatter_sum(partial):
    return lax.psum_scatter(
        partial.astype(jnp.bfloat16), "fsdp", scatter_dimension=0, tiled=True
    ).astype(jnp.float32)


class Chain:
    def __init__(self, partial, count):
        half = count // 2
        self.count = count
        self.value = partial.astype(jnp.bfloat16)
        self.flying = None
        self.hops = []
        if count % 2 == 0:
            for s in range(half - 1):
                self.hops.append(([(s, s + 1), (count - 1 - s, count - 2 - s)], None))
            self.hops.append(([(half - 1, half), (half, half - 1)], None))
            for s in reversed(range(half - 1)):
                self.hops.append(([(s + 1, s), (count - 2 - s, count - 1 - s)], s))
        elif count > 1:
            self.value = lax.psum(self.value, "sp")
        self.at = 0

    def send(self):
        if self.at < len(self.hops):
            self.flying = lax.ppermute(self.value, "sp", self.hops[self.at][0])

    def take(self):
        depth = self.hops[self.at][1]
        if depth is None:
            total = self.value.astype(jnp.float32) + self.flying.astype(jnp.float32)
            self.value = total.astype(jnp.bfloat16)
        else:
            place = lax.axis_index("sp")
            mine = jnp.minimum(place, self.count - 1 - place) == depth
            self.value = jnp.where(mine, self.flying, self.value)
        self.at += 1
        self.flying = None

    def finish(self):
        while self.at < len(self.hops):
            if self.flying is None:
                self.send()
            self.take()
        return self.value


def meet(values, moving, starting=()):
    moving = [c for c in moving if c.flying is not None]
    tied = lax.optimization_barrier(
        (values, [c.flying for c in moving], [c.value for c in starting])
    )
    for chain, arrived in zip(moving, tied[1]):
        chain.flying = arrived
        chain.take()
        chain.send()
    for chain, value in zip(starting, tied[2]):
        chain.value = value
        chain.send()
    return tied[0]


def column_blocks(array, ways):
    me = lax.axis_index("fsdp")
    half = ways // 2
    size = array.shape[1] // ways
    blocks = []
    for shift in range(ways):
        device = (me + shift) % ways
        block = 2 * (device % half) + device // half
        blocks.append(lax.dynamic_slice_in_dim(array, block * size, size, 1))
    return blocks


def turn(blocks):
    me = lax.axis_index("fsdp")
    ways = len(blocks)
    size = blocks[0].shape[0]
    result = jnp.zeros((ways * size, blocks[0].shape[1]), blocks[0].dtype)
    result = lax.dynamic_update_slice_in_dim(result, blocks[0], me * size, 0)
    for shift in range(1, ways):
        pairs = [(f, (f + shift) % ways) for f in range(ways)]
        arrived = lax.ppermute(blocks[shift], "fsdp", pairs)
        source = (me - shift) % ways
        result = lax.dynamic_update_slice_in_dim(result, arrived, source * size, 0)
    return result


def sum_all(values, sizes):
    for axis, size in sizes:
        if size & (size - 1):
            values = lax.psum(values, axis)
            continue
        step = 1
        while step < size:
            values = values + lax.ppermute(values, axis, [(d, d ^ step) for d in range(size)])
            step *= 2
    return values


def halves(array):
    middle = array.shape[0] // 2
    return (array[:middle], array[middle:])


def layer(
    ways,
    line,
    hidden_in,
    positions,
    attn_gain,
    qkv_weight,
    query_gain,
    key_gain,
    out_weight,
    mlp_gain,
    gate_up_weight,
    down_weight,
    cotangent,
):
    f32 = jnp.float32
    low = jnp.bfloat16
    rows, width = hidden_in.shape
    group = H // KV
    units = FF // ways
    pairs_of = ways // 2
    side = lax.axis_index("fsdp") // pairs_of
    swap = [(f, (f + pairs_of) % ways) for f in range(ways)]

    qkv_full = gather_rows(qkv_weight)
    kept = lax.dynamic_slice_in_dim(gate_up_weight, side * units, units, 0)
    sent = lax.dynamic_slice_in_dim(gate_up_weight, (1 - side) * units, units, 0)
    down_blocks = column_blocks(down_weight, ways)
    qkv_full, sent, down_blocks, out_late, cotangent_late = lax.optimization_barrier(
        (qkv_full, sent, down_blocks, out_weight, cotangent)
    )
    out_full = gather_rows(out_late)
    cotangent_all = gather_rows(cotangent_late)
    swapped = lax.ppermute(sent, "fsdp", swap)
    gate_up_own = jnp.concatenate([kept, swapped], 0)
    down_own = turn(down_blocks)
    hidden = hidden_in.astype(f32)
    normed1, inverse1 = rms_forward(hidden, attn_gain)
    normed1_low = normed1.astype(low)
    projected = product_nt(normed1_low, qkv_full)
    query = projected[:, : H * HD].reshape(rows, H, HD)
    key = projected[:, H * HD : (H + KV) * HD].reshape(rows, KV, HD)
    value_low = projected[:, (H + KV) * HD :].astype(low)
    cosine, sine = rotary_tables(positions)
    query_normed, query_inverse = rms_forward(query, query_gain)
    key_normed, key_inverse = rms_forward(key, key_gain)
    query_low = rotate(query_normed, cosine, sine).astype(low).reshape(rows, H * HD)
    key_low = rotate(key_normed, cosine, sine).astype(low).reshape(rows, KV * HD)
    query_heads, key_heads, value_heads = (
        lax.all_to_all(query_low, "sp", split_axis=1, concat_axis=0, tiled=True),
        lax.all_to_all(key_low, "sp", split_axis=1, concat_axis=0, tiled=True),
        lax.all_to_all(value_low, "sp", split_axis=1, concat_axis=0, tiled=True),
    )
    length = query_heads.shape[0]
    local_kv = key_heads.shape[1] // HD
    query_local = query_heads.reshape(length, -1, HD)
    keys_local = jnp.repeat(key_heads.reshape(length, local_kv, HD), group, axis=1)
    values_local = jnp.repeat(value_heads.reshape(length, local_kv, HD), group, axis=1)
    mixed_heads, logsums = attention_forward(query_local, keys_local, values_local)
    attended = lax.all_to_all(
        mixed_heads.reshape(length, -1), "sp", split_axis=0, concat_axis=1, tiled=True
    )
    middle = hidden + product_nt(attended, out_full)
    normed2, inverse2 = rms_forward(middle, mlp_gain)
    normed2_all = gather_rows(normed2.astype(low))
    normed1_late, middle = lax.optimization_barrier((normed1_low, middle))
    normed1_all = gather_rows(normed1_late)

    grad_act = jnp.dot(cotangent_all, down_own, preferred_element_type=f32)
    both = product_nt(normed2_all, gate_up_own)
    first, second = both[:, :units], both[:, units:]
    gate = jnp.where(side == 0, first, second)
    upper = jnp.where(side == 0, second, first)
    sigmoid = jax.nn.sigmoid(gate)
    activation = (gate * sigmoid * upper).astype(low)
    grad_gate = grad_act * upper * sigmoid * (1.0 + gate * (1.0 - sigmoid))
    grad_upper = grad_act * gate * sigmoid
    grad_first = jnp.where(side == 0, grad_gate, grad_upper).astype(low)
    grad_second = jnp.where(side == 0, grad_upper, grad_gate).astype(low)
    grad_both = jnp.concatenate([grad_first, grad_second], 1)
    grad_normed2 = scatter_sum(jnp.dot(grad_both, gate_up_own, preferred_element_type=f32))
    grad_sent = product_tn(grad_second, normed2_all).astype(low)
    s0, s1 = (Chain(part, line) for part in halves(grad_sent))
    s0.send()
    s1.send()
    grad_down_own = product_tn(cotangent_all, activation).astype(low)
    grad_kept = product_tn(grad_first, normed2_all).astype(low)
    grad_kept, grad_down_own = meet((grad_kept, grad_down_own), [s0])
    d0, d1 = (Chain(part, line) for part in halves(grad_down_own))
    k0, k1 = (Chain(part, line) for part in halves(grad_kept))

    back_two, mlp_term = rms_backward(middle, inverse2, mlp_gain, grad_normed2)
    grad_middle = cotangent.astype(f32) + back_two
    grad_mixed_low = grad_middle.astype(low)
    grad_attended = jnp.dot(grad_mixed_low, out_full, preferred_element_type=f32).astype(low)
    grad_heads = lax.all_to_all(grad_attended, "sp", split_axis=1, concat_axis=0, tiled=True)
    grad_mixed_low = meet(grad_mixed_low, [s1], [d0, d1])
    grad_out = scatter_sum(product_tn(grad_mixed_low, attended))
    grad_query_local, grad_keys, grad_values = attention_backward(
        query_local,
        keys_local,
        values_local,
        mixed_heads,
        logsums,
        grad_heads.reshape(length, -1, HD),
        lambda values: meet(values, [s0]),
    )
    grad_query_send = grad_query_local.astype(low).reshape(length, -1)
    grad_key_send = (
        grad_keys.reshape(length, local_kv, group, HD).sum(2).astype(low).reshape(length, -1)
    )
    grad_value_send = (
        grad_values.reshape(length, local_kv, group, HD).sum(2).astype(low).reshape(length, -1)
    )
    grads_send = jnp.concatenate([grad_query_send, grad_key_send, grad_value_send], 1)
    grads_send, activation = meet((grads_send, activation), [s1, d0], [k0, k1])
    grads_low = lax.all_to_all(grads_send, "sp", split_axis=0, concat_axis=1, tiled=True)
    hidden_out = (middle + scatter_sum(product_nt(activation, down_own))).astype(low)
    grads_low = meet(grads_low, [d1])
    grads_low = grads_low.reshape(rows, line, -1)
    cuts = (grad_query_send.shape[1], grad_query_send.shape[1] + grad_key_send.shape[1])
    grad_query_low = grads_low[:, :, : cuts[0]]
    grad_key_low = grads_low[:, :, cuts[0] : cuts[1]]
    grad_value_low = grads_low[:, :, cuts[1] :].reshape(rows, KV * HD)
    grad_query, query_term = rms_backward(
        query,
        query_inverse,
        query_gain,
        rotate_back(grad_query_low.astype(f32).reshape(rows, H, HD), cosine, sine),
    )
    grad_query, query_term = meet((grad_query, query_term), [d0, k0])
    grad_key, key_term = rms_backward(
        key,
        key_inverse,
        key_gain,
        rotate_back(grad_key_low.astype(f32).reshape(rows, KV, HD), cosine, sine),
    )
    grad_projected = jnp.concatenate(
        [
            grad_query.reshape(rows, H * HD).astype(low),
            grad_key.reshape(rows, KV * HD).astype(low),
            grad_value_low,
        ],
        1,
    )
    grad_columns = lax.all_to_all(grad_projected, "fsdp", split_axis=1, concat_axis=0, tiled=True)
    out_chain = Chain(grad_out, line)
    grad_columns = meet(grad_columns, [d1, k0, k1, s0, s1], [out_chain])
    swapped_back = []
    for chain in (s0, s1):
        swapped_back.append(lax.ppermute(chain.finish(), "fsdp", swap))
    grad_normed1 = jnp.dot(grad_projected, qkv_full, preferred_element_type=f32)
    grad_qkv_own = product_tn(grad_columns, normed1_all).astype(low)
    back_one, attn_term = rms_backward(hidden, inverse1, attn_gain, grad_normed1)
    grad_input = grad_middle + back_one
    terms = jnp.concatenate(
        [
            jnp.sum(attn_term, axis=0),
            jnp.sum(mlp_term, axis=0),
            jnp.sum(query_term, axis=(0, 1)),
            jnp.sum(key_term, axis=(0, 1)),
        ]
    )
    grad_qkv_own, terms = meet((grad_qkv_own, terms), [])
    q0, q1 = (Chain(part, line) for part in halves(grad_qkv_own))
    q0.send()
    q1.send()
    meet((), [out_chain])
    meet((), [k1])
    swapped_back = [meet(swapped_back[0], [q0, d0]), meet(swapped_back[1], [q1])]
    grad_swapped = jnp.concatenate(swapped_back, 0)
    grad_down_sum = jnp.concatenate([d0.finish(), d1.finish()], 0)
    down_back = lax.all_to_all(
        grad_down_sum.reshape(ways, -1, units),
        "fsdp",
        split_axis=0,
        concat_axis=0,
        tiled=True,
    )
    columns = [
        down_back[(b % 2) * pairs_of + b // 2] for b in range(ways)
    ]
    grad_down = jnp.concatenate(columns, 1).astype(f32)
    grad_down, terms = meet((grad_down, terms), [])
    sums = sum_all(terms, (("fsdp", ways), ("sp", line)))
    grad_kept = jnp.concatenate([k0.finish(), k1.finish()], 0)
    grad_gate_up = jnp.concatenate(
        [
            jnp.where(side == 0, grad_kept, grad_swapped),
            jnp.where(side == 0, grad_swapped, grad_kept),
        ],
        0,
    ).astype(f32)
    grad_out = out_chain.finish().astype(f32)
    grad_qkv = jnp.concatenate([q0.finish(), q1.finish()], 0).astype(f32)
    gains = (
        sums[:width],
        sums[2 * width : 2 * width + HD],
        sums[2 * width + HD :],
        sums[width : 2 * width],
    )
    return (
        hidden_out,
        grad_input,
        gains[0],
        grad_qkv,
        gains[1],
        gains[2],
        grad_out,
        gains[3],
        grad_gate_up,
        grad_down,
    )


def solution(mesh):
    return jax.shard_map(
        functools.partial(layer, mesh.shape["fsdp"], mesh.shape["sp"]),
        mesh=mesh,
        in_specs=(
            P(("fsdp", "sp"), None),
            P(("fsdp", "sp")),
            P(),
            P("fsdp", None),
            P(),
            P(),
            P("fsdp", None),
            P(),
            P("fsdp", None),
            P("fsdp", None),
            P(("fsdp", "sp"), None),
        ),
        out_specs=(
            P(("fsdp", "sp"), None),
            P(("fsdp", "sp"), None),
            P(),
            P("fsdp", None),
            P(),
            P(),
            P("fsdp", None),
            P(),
            P("fsdp", None),
            P("fsdp", None),
        ),
        check_vma=False,
    )
```

```python
import functools

import jax
import jax.numpy as jnp
from jax import lax
from jax.sharding import PartitionSpec as P


H = 16
KV = 8
HD = 128
FF = 6144


EPS = 1e-06
THETA = 1000000.0
NEGATIVE = -1e30


def rms_forward(values, gain):
    inverse = lax.rsqrt(jnp.mean(values * values, axis=-1, keepdims=True) + EPS)
    return (values * inverse * gain, inverse)


def rms_backward(values, inverse, gain, upstream):
    scaled = upstream * gain
    cubed = inverse * inverse * inverse
    gradient = inverse * scaled - values * cubed * jnp.mean(scaled * values, axis=-1, keepdims=True)
    return (gradient, upstream * values * inverse)


def rotary_tables(positions):
    half = HD // 2
    frequency = THETA ** (-(jnp.arange(half, dtype=jnp.float32) * 2.0 / HD))
    angle = positions.astype(jnp.float32)[:, None] * frequency[None, :]
    cosine = jnp.cos(angle)
    sine = jnp.sin(angle)
    return (
        jnp.concatenate([cosine, cosine], -1)[:, None, :],
        jnp.concatenate([sine, sine], -1)[:, None, :],
    )


def rotate(values, cosine, sine):
    half = HD // 2
    turned = jnp.concatenate([-values[..., half:], values[..., :half]], -1)
    return values * cosine + turned * sine


def rotate_back(gradient, cosine, sine):
    half = HD // 2
    scaled = gradient * sine
    return gradient * cosine + jnp.concatenate([scaled[..., half:], -scaled[..., :half]], -1)


def scores_block(query_block, keys, start):
    scores = jnp.einsum("qhd,khd->hqk", query_block, keys, preferred_element_type=jnp.float32)
    query_rows = start + jnp.arange(query_block.shape[0])
    key_rows = jnp.arange(keys.shape[0])
    allowed = key_rows[None, :] <= query_rows[:, None]
    return jnp.where(allowed[None], scores * HD ** (-0.5), NEGATIVE)


def blocks_of(length):
    block = min(512, length)
    return [(start, start + block) for start in range(0, length, block)]


def attention_forward(query, keys, values):
    mixed_all, logsums = [], []
    for start, stop in blocks_of(query.shape[0]):
        scores = scores_block(query[start:stop], keys[:stop], start)
        top = jnp.max(scores, axis=-1, keepdims=True)
        logsum = top + jnp.log(jnp.sum(jnp.exp(scores - top), axis=-1, keepdims=True))
        weights = jnp.exp(scores - logsum).astype(jnp.bfloat16)
        mixed = jnp.einsum(
            "hqk,khd->qhd", weights, values[:stop], preferred_element_type=jnp.float32
        )
        mixed_all.append(mixed.astype(jnp.bfloat16))
        logsums.append(logsum)
    return (jnp.concatenate(mixed_all, 0), logsums)


def attention_backward(query, keys, values, mixed_all, logsums, grad_mixed, between):
    length = query.shape[0]
    factor = HD ** (-0.5)
    grad_query, key_total, value_total = [], None, None
    for (start, stop), logsum in reversed(list(zip(blocks_of(length), logsums))):
        query_block = query[start:stop]
        grad_block = grad_mixed[start:stop]
        mixed_block = mixed_all[start:stop]
        scores = scores_block(query_block, keys[:stop], start)
        chances = jnp.exp(scores - logsum)
        weights_low = chances.astype(jnp.bfloat16)
        delta = jnp.sum(grad_block.astype(jnp.float32) * mixed_block.astype(jnp.float32), axis=-1)
        grad_weights = jnp.einsum(
            "qhd,khd->hqk", grad_block, values[:stop], preferred_element_type=jnp.float32
        )
        grad_scores = (chances * (grad_weights - delta.T[:, :, None])).astype(jnp.bfloat16)
        grad_query.append(
            jnp.einsum(
                "hqk,khd->qhd", grad_scores, keys[:stop], preferred_element_type=jnp.float32
            )
            * factor
        )
        key_part = (
            jnp.einsum("hqk,qhd->khd", grad_scores, query_block, preferred_element_type=jnp.float32)
            * factor
        )
        value_part = jnp.einsum(
            "hqk,qhd->khd", weights_low, grad_block, preferred_element_type=jnp.float32
        )
        if key_total is None:
            key_total, value_total = key_part, value_part
            grad_mixed, key_total = between((grad_mixed, key_total))
        else:
            key_total = key_total.at[:stop].add(key_part)
            value_total = value_total.at[:stop].add(value_part)
    return (jnp.concatenate(grad_query[::-1], 0), key_total, value_total)


def gather_rows(array):
    return lax.all_gather(array, "fsdp", axis=0, tiled=True)


def product_nt(inputs, weight):
    return lax.dot_general(
        inputs, weight, (((1,), (1,)), ((), ())), preferred_element_type=jnp.float32
    )


def product_tn(left, right):
    return lax.dot_general(
        left, right, (((0,), (0,)), ((), ())), preferred_element_type=jnp.float32
    )


def scatter_sum(partial):
    return lax.psum_scatter(
        partial.astype(jnp.bfloat16), "fsdp", scatter_dimension=0, tiled=True
    ).astype(jnp.float32)


class Chain:
    def __init__(self, partial, count):
        half = count // 2
        self.count = count
        self.value = partial.astype(jnp.bfloat16)
        self.flying = None
        self.hops = []
        if count % 2 == 0:
            for s in range(half - 1):
                self.hops.append(([(s, s + 1), (count - 1 - s, count - 2 - s)], None))
            self.hops.append(([(half - 1, half), (half, half - 1)], None))
            for s in reversed(range(half - 1)):
                self.hops.append(([(s + 1, s), (count - 2 - s, count - 1 - s)], s))
        elif count > 1:
            self.value = lax.psum(self.value, "sp")
        self.at = 0

    def send(self):
        if self.at < len(self.hops):
            self.flying = lax.ppermute(self.value, "sp", self.hops[self.at][0])

    def take(self):
        depth = self.hops[self.at][1]
        if depth is None:
            total = self.value.astype(jnp.float32) + self.flying.astype(jnp.float32)
            self.value = total.astype(jnp.bfloat16)
        else:
            place = lax.axis_index("sp")
            mine = jnp.minimum(place, self.count - 1 - place) == depth
            self.value = jnp.where(mine, self.flying, self.value)
        self.at += 1
        self.flying = None

    def finish(self):
        while self.at < len(self.hops):
            if self.flying is None:
                self.send()
            self.take()
        return self.value


def meet(values, moving, starting=()):
    moving = [c for c in moving if c.flying is not None]
    tied = lax.optimization_barrier(
        (values, [c.flying for c in moving], [c.value for c in starting])
    )
    for chain, arrived in zip(moving, tied[1]):
        chain.flying = arrived
        chain.take()
        chain.send()
    for chain, value in zip(starting, tied[2]):
        chain.value = value
        chain.send()
    return tied[0]


def column_blocks(array, ways):
    me = lax.axis_index("fsdp")
    half = ways // 2
    size = array.shape[1] // ways
    blocks = []
    for shift in range(ways):
        device = (me + shift) % ways
        block = 2 * (device % half) + device // half
        blocks.append(lax.dynamic_slice_in_dim(array, block * size, size, 1))
    return blocks


def turn(blocks):
    me = lax.axis_index("fsdp")
    ways = len(blocks)
    size = blocks[0].shape[0]
    result = jnp.zeros((ways * size, blocks[0].shape[1]), blocks[0].dtype)
    result = lax.dynamic_update_slice_in_dim(result, blocks[0], me * size, 0)
    for shift in range(1, ways):
        pairs = [(f, (f + shift) % ways) for f in range(ways)]
        arrived = lax.ppermute(blocks[shift], "fsdp", pairs)
        source = (me - shift) % ways
        result = lax.dynamic_update_slice_in_dim(result, arrived, source * size, 0)
    return result


def sum_all(values, sizes):
    for axis, size in sizes:
        if size & (size - 1):
            values = lax.psum(values, axis)
            continue
        step = 1
        while step < size:
            values = values + lax.ppermute(values, axis, [(d, d ^ step) for d in range(size)])
            step *= 2
    return values


def halves(array):
    middle = array.shape[0] // 2
    return (array[:middle], array[middle:])


def layer(
    ways,
    line,
    hidden_in,
    positions,
    attn_gain,
    qkv_weight,
    query_gain,
    key_gain,
    out_weight,
    mlp_gain,
    gate_up_weight,
    down_weight,
    cotangent,
):
    f32 = jnp.float32
    low = jnp.bfloat16
    rows, width = hidden_in.shape
    group = H // KV
    units = FF // ways
    pairs_of = ways // 2
    side = lax.axis_index("fsdp") // pairs_of
    swap = [(f, (f + pairs_of) % ways) for f in range(ways)]

    qkv_full = gather_rows(qkv_weight)
    kept = lax.dynamic_slice_in_dim(gate_up_weight, side * units, units, 0)
    sent = lax.dynamic_slice_in_dim(gate_up_weight, (1 - side) * units, units, 0)
    down_blocks = column_blocks(down_weight, ways)
    qkv_full, sent, down_blocks, out_late, cotangent_late = lax.optimization_barrier(
        (qkv_full, sent, down_blocks, out_weight, cotangent)
    )
    out_full = gather_rows(out_late)
    cotangent_all = gather_rows(cotangent_late)
    swapped = lax.ppermute(sent, "fsdp", swap)
    gate_up_own = jnp.concatenate([kept, swapped], 0)
    down_own = turn(down_blocks)
    hidden = hidden_in.astype(f32)
    normed1, inverse1 = rms_forward(hidden, attn_gain)
    normed1_low = normed1.astype(low)
    projected = product_nt(normed1_low, qkv_full)
    query = projected[:, : H * HD].reshape(rows, H, HD)
    key = projected[:, H * HD : (H + KV) * HD].reshape(rows, KV, HD)
    value_low = projected[:, (H + KV) * HD :].astype(low)
    cosine, sine = rotary_tables(positions)
    query_normed, query_inverse = rms_forward(query, query_gain)
    key_normed, key_inverse = rms_forward(key, key_gain)
    query_low = rotate(query_normed, cosine, sine).astype(low).reshape(rows, H * HD)
    key_low = rotate(key_normed, cosine, sine).astype(low).reshape(rows, KV * HD)
    query_heads, key_heads, value_heads = (
        lax.all_to_all(query_low, "sp", split_axis=1, concat_axis=0, tiled=True),
        lax.all_to_all(key_low, "sp", split_axis=1, concat_axis=0, tiled=True),
        lax.all_to_all(value_low, "sp", split_axis=1, concat_axis=0, tiled=True),
    )
    length = query_heads.shape[0]
    local_kv = key_heads.shape[1] // HD
    query_local = query_heads.reshape(length, -1, HD)
    keys_local = jnp.repeat(key_heads.reshape(length, local_kv, HD), group, axis=1)
    values_local = jnp.repeat(value_heads.reshape(length, local_kv, HD), group, axis=1)
    mixed_heads, logsums = attention_forward(query_local, keys_local, values_local)
    attended = lax.all_to_all(
        mixed_heads.reshape(length, -1), "sp", split_axis=0, concat_axis=1, tiled=True
    )
    middle = hidden + product_nt(attended, out_full)
    normed2, inverse2 = rms_forward(middle, mlp_gain)
    normed2_all = gather_rows(normed2.astype(low))
    normed1_late, middle = lax.optimization_barrier((normed1_low, middle))
    normed1_all = gather_rows(normed1_late)

    grad_act = jnp.dot(cotangent_all, down_own, preferred_element_type=f32)
    grad_act = lax.optimization_barrier(grad_act)
    both = product_nt(normed2_all, gate_up_own)
    first, second = both[:, :units], both[:, units:]
    gate = jnp.where(side == 0, first, second)
    upper = jnp.where(side == 0, second, first)
    sigmoid = jax.nn.sigmoid(gate)
    activation = (gate * sigmoid * upper).astype(low)
    grad_gate = grad_act * upper * sigmoid * (1.0 + gate * (1.0 - sigmoid))
    grad_upper = grad_act * gate * sigmoid
    grad_first = jnp.where(side == 0, grad_gate, grad_upper).astype(low)
    grad_second = jnp.where(side == 0, grad_upper, grad_gate).astype(low)
    grad_both = jnp.concatenate([grad_first, grad_second], 1)
    grad_normed2 = scatter_sum(jnp.dot(grad_both, gate_up_own, preferred_element_type=f32))
    grad_sent = product_tn(grad_second, normed2_all).astype(low)
    s0, s1 = (Chain(part, line) for part in halves(grad_sent))
    s0.send()
    s1.send()
    grad_down_own = product_tn(cotangent_all, activation).astype(low)
    grad_kept = product_tn(grad_first, normed2_all).astype(low)
    grad_kept, grad_down_own = meet((grad_kept, grad_down_own), [s0])
    d0, d1 = (Chain(part, line) for part in halves(grad_down_own))
    k0, k1 = (Chain(part, line) for part in halves(grad_kept))

    back_two, mlp_term = rms_backward(middle, inverse2, mlp_gain, grad_normed2)
    grad_middle = cotangent.astype(f32) + back_two
    grad_mixed_low = grad_middle.astype(low)
    grad_attended = jnp.dot(grad_mixed_low, out_full, preferred_element_type=f32).astype(low)
    grad_heads = lax.all_to_all(grad_attended, "sp", split_axis=1, concat_axis=0, tiled=True)
    grad_mixed_low = meet(grad_mixed_low, [s1], [d0, d1])
    grad_out = scatter_sum(product_tn(grad_mixed_low, attended))
    grad_query_local, grad_keys, grad_values = attention_backward(
        query_local,
        keys_local,
        values_local,
        mixed_heads,
        logsums,
        grad_heads.reshape(length, -1, HD),
        lambda values: meet(values, [s0]),
    )
    grad_query_send = grad_query_local.astype(low).reshape(length, -1)
    grad_key_send = (
        grad_keys.reshape(length, local_kv, group, HD).sum(2).astype(low).reshape(length, -1)
    )
    grad_value_send = (
        grad_values.reshape(length, local_kv, group, HD).sum(2).astype(low).reshape(length, -1)
    )
    grads_send = jnp.concatenate([grad_query_send, grad_key_send, grad_value_send], 1)
    grads_send, activation = meet((grads_send, activation), [s1, d0], [k0, k1])
    grads_low = lax.all_to_all(grads_send, "sp", split_axis=0, concat_axis=1, tiled=True)
    hidden_out = (middle + scatter_sum(product_nt(activation, down_own))).astype(low)
    out_chain = Chain(grad_out, line)
    grads_low = meet(grads_low, [d1], [out_chain])
    grads_low = grads_low.reshape(rows, line, -1)
    cuts = (grad_query_send.shape[1], grad_query_send.shape[1] + grad_key_send.shape[1])
    grad_query_low = grads_low[:, :, : cuts[0]]
    grad_key_low = grads_low[:, :, cuts[0] : cuts[1]]
    grad_value_low = grads_low[:, :, cuts[1] :].reshape(rows, KV * HD)
    grad_query, query_term = rms_backward(
        query,
        query_inverse,
        query_gain,
        rotate_back(grad_query_low.astype(f32).reshape(rows, H, HD), cosine, sine),
    )
    grad_query, query_term = meet((grad_query, query_term), [d0, k0])
    grad_key, key_term = rms_backward(
        key,
        key_inverse,
        key_gain,
        rotate_back(grad_key_low.astype(f32).reshape(rows, KV, HD), cosine, sine),
    )
    grad_projected = jnp.concatenate(
        [
            grad_query.reshape(rows, H * HD).astype(low),
            grad_key.reshape(rows, KV * HD).astype(low),
            grad_value_low,
        ],
        1,
    )
    grad_columns = lax.all_to_all(grad_projected, "fsdp", split_axis=1, concat_axis=0, tiled=True)
    grad_columns = meet(grad_columns, [d1, k0, k1, s0, s1, out_chain])
    swapped_back = []
    for chain in (s0, s1):
        swapped_back.append(lax.ppermute(chain.finish(), "fsdp", swap))
    grad_normed1 = jnp.dot(grad_projected, qkv_full, preferred_element_type=f32)
    grad_qkv_own = product_tn(grad_columns, normed1_all).astype(low)
    back_one, attn_term = rms_backward(hidden, inverse1, attn_gain, grad_normed1)
    grad_input = grad_middle + back_one
    terms = jnp.concatenate(
        [
            jnp.sum(attn_term, axis=0),
            jnp.sum(mlp_term, axis=0),
            jnp.sum(query_term, axis=(0, 1)),
            jnp.sum(key_term, axis=(0, 1)),
        ]
    )
    grad_qkv_own, terms = meet((grad_qkv_own, terms), [])
    q0, q1 = (Chain(part, line) for part in halves(grad_qkv_own))
    q0.send()
    q1.send()
    meet((), [out_chain])
    meet((), [k1])
    swapped_back = [meet(swapped_back[0], [q0, d0]), meet(swapped_back[1], [q1])]
    grad_swapped = jnp.concatenate(swapped_back, 0)
    grad_down_sum = jnp.concatenate([d0.finish(), d1.finish()], 0)
    down_back = lax.all_to_all(
        grad_down_sum.reshape(ways, -1, units),
        "fsdp",
        split_axis=0,
        concat_axis=0,
        tiled=True,
    )
    columns = [
        down_back[(b % 2) * pairs_of + b // 2] for b in range(ways)
    ]
    grad_down = jnp.concatenate(columns, 1).astype(f32)
    grad_down, terms = meet((grad_down, terms), [])
    sums = sum_all(terms, (("fsdp", ways), ("sp", line)))
    grad_kept = jnp.concatenate([k0.finish(), k1.finish()], 0)
    grad_gate_up = jnp.concatenate(
        [
            jnp.where(side == 0, grad_kept, grad_swapped),
            jnp.where(side == 0, grad_swapped, grad_kept),
        ],
        0,
    ).astype(f32)
    grad_out = out_chain.finish().astype(f32)
    grad_qkv = jnp.concatenate([q0.finish(), q1.finish()], 0).astype(f32)
    gains = (
        sums[:width],
        sums[2 * width : 2 * width + HD],
        sums[2 * width + HD :],
        sums[width : 2 * width],
    )
    return (
        hidden_out,
        grad_input,
        gains[0],
        grad_qkv,
        gains[1],
        gains[2],
        grad_out,
        gains[3],
        grad_gate_up,
        grad_down,
    )


def solution(mesh):
    return jax.shard_map(
        functools.partial(layer, mesh.shape["fsdp"], mesh.shape["sp"]),
        mesh=mesh,
        in_specs=(
            P(("fsdp", "sp"), None),
            P(("fsdp", "sp")),
            P(),
            P("fsdp", None),
            P(),
            P(),
            P("fsdp", None),
            P(),
            P("fsdp", None),
            P("fsdp", None),
            P(("fsdp", "sp"), None),
        ),
        out_specs=(
            P(("fsdp", "sp"), None),
            P(("fsdp", "sp"), None),
            P(),
            P("fsdp", None),
            P(),
            P(),
            P("fsdp", None),
            P(),
            P("fsdp", None),
            P("fsdp", None),
        ),
        check_vma=False,
    )
```
